128 devices in a mesh: dp: 8 (over z_hi, x), expert: 16 (over y, z_lo, core).
Axes of the slice: x: 4, y: 4, z: 4 (z_hi: 2, z_lo: 2; z = z_hi * 2 + z_lo), core: 2. Of those that a mesh axis runs over, the one named last changes fastest.
Arguments:
- tokens: bfloat16 [32768, 2048], P(('dp', 'expert')), may hold values from -6 to 6
- expert_ids: int32 [32768, 8], P(('dp', 'expert')), may hold values from 0 to 31, all different within a row; in each aligned block of 256 rows (0 to 255, 256 to 511, ...) at most 80 rows name the same one
- route_probs: float32 [32768, 8], P(('dp', 'expert')), may hold values from 0.05 to 1
- w_gate_up: bfloat16 [32, 2048, 1536], P('expert', 'dp'), may hold values from -0.125 to 0.125
- w_down: bfloat16 [32, 768, 2048], P('expert', None, 'dp'), may hold values from -0.21875 to 0.21875
Outputs:
- moe_out: bfloat16 [32768, 2048], P(('dp', 'expert'))
The draws below stay inside these ranges and needn't reach their ends.
Inputs may be any that keep to these rules, and one draw needn't show every extreme that they name: `expert_ids`: each row names 8 different experts. Among the rows of one device no expert is named more than 80 times, and in every draw some expert is named exactly 80 times in some device's rows.
All inputs are finite; a program needn't handle non-finite values.
Results may differ from the reference program's by a relative error of at most 0.0057.
Values may be sent and summed in bfloat16 or wider, within the bound.
A program may use at most 128 MiB of HBM per device.

```python
import math
import jax
import jax.numpy as jnp
import numpy as np
from jax import lax

D = 2048
FF = 768
TOP = 8
TOK_DEV = 256
EXPERTS = 32
CAP = 80
TOKENS = 32768


def levels(rng, dims, split, smallest, high):
    gain = 1.0
    for axis_at, blocks in split:
        heights = jax.random.uniform(jax.random.fold_in(jax.random.fold_in(rng, 6), axis_at), (blocks,), jnp.float32, smallest / len(split), high / len(split))
        gain = gain * jnp.repeat(jnp.exp(heights), dims[axis_at] // blocks).reshape((-1,) + (1,) * (len(dims) - 1 - axis_at))
    return gain


def deal_out(stream_key, own, number, rows, count, top, limit, lean):
    sequence = jax.random.permutation(stream_key, count)
    packed, usual = shares(count, rows * top, limit, lean, True), shares(count, rows * top, limit, lean, False)
    places = jnp.arange(count)

    def named(sizes, offset_by):
        used = int((sizes > 0).sum())
        fixed = max(1, used // 4)
        shifted = fixed + (places - fixed + offset_by * (used - fixed)) % max(1, count - fixed)
        return jnp.zeros((count,), jnp.int32).at[sequence[jnp.where(places < fixed, places, shifted)]].set(jnp.asarray(sizes, jnp.int32))

    sizes = jnp.where(number % 4 == 0, named(packed, number // 4), named(usual, number - number // 4 - 1))
    mixed = jax.random.permutation(jax.random.fold_in(own, 3), count)
    source_of, taker = mixed[0:count // 2 * 2:2], mixed[1:count // 2 * 2:2]
    margin = jnp.minimum(sizes[source_of] - 1, limit - sizes[taker]) // 2
    margin = jnp.where((source_of == sequence[0]) | (taker == sequence[0]) | (sizes[taker] == 0), 0, jnp.maximum(margin, 0))
    shifted = jax.random.randint(jax.random.fold_in(own, 4), (count // 2,), 0, 1 << 20) % (margin + 1)
    sizes = sizes.at[source_of].add(-shifted).at[taker].add(shifted)
    labels = jnp.searchsorted(jnp.cumsum(sizes), jnp.arange(rows * top), side="right").astype(jnp.int32)
    listing = labels.reshape(top, rows).T
    listing = listing[jax.random.permutation(jax.random.fold_in(own, 1), rows)]
    offset_by = jax.random.randint(jax.random.fold_in(own, 2), (rows, 1), 0, top)
    return jnp.take_along_axis(listing, (jnp.arange(top)[None, :] + offset_by) % top, axis=1)


def shares(amount, total, reach, lean, full):
    loads = [(1 << 20) // math.isqrt(rank ** lean) + 1 for rank in range(1, amount + 1)]
    largest = reach if full else min(reach, max(-(-total // amount), total * loads[0] // sum(loads)))
    least = 1 if total - largest >= amount - 1 else 0
    given, rest = [largest] + [least] * (amount - 1), total - largest - least * (amount - 1)
    while rest > 0:
        movable = [i for i in range(1, amount) if given[i] < largest] or [i for i in range(1, amount) if given[i] < reach]
        mass, remaining = sum([loads[i] for i in movable]), rest
        for i in movable:
            more = min(reach - given[i], max(1, remaining * loads[i] // mass), rest)
            given[i] = given[i] + more
            rest = rest - more
    return np.array(given)


def normal_values(key, extent, width, reach, shards=(), kind=jnp.bfloat16):
    loudness = levels(key, extent, shards, -0.22, 0.18) if shards else 1.0
    array = jax.random.normal(key, extent, jnp.float32) * width * loudness
    return jnp.minimum(jnp.maximum(array, -reach), reach).astype(kind)


def setup_inputs(seed: int = 0) -> dict:
    arg_keys = jax.random.split(jax.random.key(seed), 6)
    tokens = normal_values(arg_keys[0], (TOKENS, D), 1.0, 6.0, ((0, 128),))
    expert_ids_keys = jax.random.split(jax.random.fold_in(arg_keys[1], 1), TOKENS // TOK_DEV)
    expert_ids_turns = jax.random.permutation(jax.random.fold_in(arg_keys[1], 3), TOKENS // TOK_DEV)
    expert_ids = jax.vmap(lambda own, number: deal_out(jax.random.fold_in(arg_keys[1], 2), own, number, TOK_DEV, EXPERTS, TOP, CAP, 1))(expert_ids_keys, expert_ids_turns).reshape((TOKENS, TOP))
    route_probs = jnp.clip(jnp.exp(math.log(1.0) - 2.9957323 * jax.random.uniform(arg_keys[2], (TOKENS, TOP), jnp.float32) ** levels(arg_keys[2], (TOKENS, TOP), ((0, 128),), -0.2, 0.2)), 0.05, 1.0)
    w_gate_up = normal_values(arg_keys[3], (EXPERTS, D, 2 * FF), D ** -0.5, 0.125, ((0, 16), (1, 8)))
    w_down = normal_values(arg_keys[4], (EXPERTS, FF, D), FF ** -0.5, 0.21875, ((0, 16), (2, 8)))
    return {"tokens": tokens, "expert_ids": expert_ids, "route_probs": route_probs, "w_gate_up": w_gate_up, "w_down": w_down}


def reference(tokens, expert_ids, route_probs, w_gate_up, w_down):
    experts = w_gate_up.shape[0]
    device_count = tokens.shape[0] // TOK_DEV
    slots_all = device_count * CAP
    weights = route_probs / jnp.sum(route_probs, axis=1, keepdims=True)
    blocks = expert_ids.reshape(device_count, TOK_DEV * TOP).astype(jnp.int32)
    onehot = (blocks[:, :, None] == jnp.arange(experts, dtype=jnp.int32)[None, None, :]).astype(jnp.int32)
    before = jnp.cumsum(onehot, axis=1) - onehot
    slot_of = jnp.sum(before * onehot, axis=2).astype(jnp.int32)
    device_of = jnp.arange(device_count, dtype=jnp.int32)[:, None]
    position = (blocks * slots_all + device_of * CAP + slot_of).reshape(-1).astype(jnp.int32)
    token_of = (device_of * TOK_DEV + jnp.arange(TOK_DEV * TOP, dtype=jnp.int32)[None, :] // TOP).reshape(-1).astype(jnp.int32)
    row_table = jnp.zeros((experts * slots_all,), jnp.int32).at[position].set(token_of).reshape(experts, slots_all)
    row_weight = jnp.zeros((experts * slots_all,), jnp.float32).at[position].set(weights.reshape(-1).astype(jnp.float32)).reshape(experts, slots_all)

    def expert_step(running, inputs):
        rows_index, rows_scale, gate_up, down = inputs
        rows_in = tokens[rows_index]
        joined = jnp.dot(rows_in, gate_up, preferred_element_type=jnp.float32)
        hidden = (jax.nn.silu(joined[:, :FF]) * joined[:, FF:]).astype(jnp.bfloat16)
        result = jnp.dot(hidden, down, preferred_element_type=jnp.float32).astype(jnp.bfloat16)
        result = lax.optimization_barrier(result).astype(jnp.float32)
        return running.at[rows_index].add(result * rows_scale[:, None]), None

    start_sum = jnp.zeros(tokens.shape, jnp.float32)
    summed, unused = lax.scan(expert_step, start_sum, (row_table, row_weight, w_gate_up, w_down))
    return summed.astype(jnp.bfloat16)
```

```python
import jax
import jax.numpy as jnp
from jax import lax
from jax.experimental import pallas as pl
from jax.experimental.pallas import tpu as pltpu
from jax.sharding import PartitionSpec as P

MESH = pl.DeviceIdType.MESH
F32 = jnp.float32
BF16 = jnp.bfloat16

TOK = 256
META = 16
ROWS = TOK + META
HALF = 144
D = 2048
FF = 768
TOP = 8
CAP = 80
SRC = 16
COL = 256
STEPS = 8
MOVES = 17 + 4 * 9 + 2 * 8 + 2 * 9

OWN, ZED, LEFT, RIGHT, ACROSS, ZLEFT, ZRIGHT, ZACROSS = range(0, 16, 2)
RETURN = {
    (0, 0): OWN, (0, 1): ZED, (1, 0): RIGHT, (1, 1): ZRIGHT,
    (2, 0): ACROSS, (2, 1): ZACROSS, (3, 0): LEFT, (3, 1): ZLEFT,
}
PIECES = [(e, n) for e in range(2) for n in range(3)]
Z_FIRST = (0, 1, 2, 3)
X_FIRST = (4, 5)


def kernel(
    tok, ids, probs, wgu, wdn, out,
    tokb, wg, wd, xs, hid, pt, yb, tri, zbuf,
    local_sem, send_sem, recv_sem, ret_send, ret_recv, free_sem,
):
    dp, ex = lax.axis_index("dp"), lax.axis_index("expert")
    zh, x = dp // 4, dp % 4
    y, zl, core = ex // 4, (ex // 2) % 2, ex % 2
    xl, xr, xa = (x + 3) % 4, (x + 1) % 4, (x + 2) % 4

    def at_dp(zhi, xx):
        return (zhi * 4 + xx, ex)

    def at_ex(yy, zz, cc):
        return (dp, (yy * 2 + zz) * 2 + cc)

    x_right, x_left, z_far = at_dp(zh, xr), at_dp(zh, xl), at_dp(1 - zh, x)
    y_right, y_left = at_ex((y + 1) % 4, zl, core), at_ex((y + 3) % 4, zl, core)
    z_near, twin = at_ex(y, 1 - zl, core), at_ex(y, zl, 1 - core)

    count = [0]

    class Move:
        def __init__(self, src, dst, device, lands=None):
            n = count[0]
            count[0] += 1
            sems = dict(send_sem=send_sem.at[n], recv_sem=recv_sem.at[n], device_id=device, device_id_type=MESH)
            lands = dst if lands is None else lands
            self.out = lambda: pltpu.make_async_remote_copy(src_ref=src, dst_ref=dst, **sems)
            self.into = lambda: pltpu.make_async_remote_copy(src_ref=lands, dst_ref=lands, **sems)

        def start(self):
            self.out().start()

        def wait_send(self):
            self.out().wait_send()

        def wait_recv(self):
            self.into().wait_recv()

    def start(*moves):
        for m in moves:
            m.start()

    def wait(*moves):
        for m in moves:
            m.wait_recv()

    first, second = pl.ds(0, HALF), pl.ds(HALF, ROWS - HALF)

    def block(src, dst, device, rows=None):
        if rows is None:
            return Move(tokb.at[src], tokb.at[dst], device)
        return Move(tokb.at[src, rows], tokb.at[dst, rows], device)

    t_z = block(OWN, ZED, z_near)
    t_right, t_left = block(OWN, LEFT, y_right), block(OWN, RIGHT, y_left)
    t_fwd_r, t_fwd_l = block(LEFT, ACROSS, y_right, first), block(RIGHT, ACROSS, y_left, second)
    t_zright, t_zleft = block(ZED, ZLEFT, y_right), block(ZED, ZRIGHT, y_left)
    t_zfwd_r, t_zfwd_l = block(ZLEFT, ZACROSS, y_right, first), block(ZRIGHT, ZACROSS, y_left, second)
    twins = {s: block(s, s + 1, twin) for s in range(0, SRC, 2)}
    token_moves = [t_z, t_right, t_left, t_fwd_r, t_fwd_l, t_zright, t_zleft, t_zfwd_r, t_zfwd_l, *twins.values()]

    def gate_up_moves(e, n, x_first):
        def move(device, sends, takes, rows=None):
            src, lands = wg.at[e, n, sends[0] * 4 + sends[1]], wg.at[e, n, takes[0] * 4 + takes[1]]
            if rows is not None:
                src, lands = src.at[rows], lands.at[rows]
            return Move(src, src, device, lands)

        top, low = pl.ds(0, COL // 2), pl.ds(COL // 2, COL // 2)
        far = 1 - zh
        moves = dict(
            right=move(x_right, (zh, x), (zh, xl)), left=move(x_left, (zh, x), (zh, xr)),
            fwd_r=move(x_right, (zh, xl), (zh, xa), top), fwd_l=move(x_left, (zh, xr), (zh, xa), low),
            z=move(z_far, (zh, x), (far, x)),
        )
        if x_first:
            moves.update(
                zl=move(z_far, (zh, xl), (far, xl)), zr=move(z_far, (zh, xr), (far, xr)),
                za=move(z_far, (zh, xa), (far, xa)),
            )
        else:
            moves.update(
                zright=move(x_right, (far, x), (far, xl)), zleft=move(x_left, (far, x), (far, xr)),
                zfwd_r=move(x_right, (far, xl), (far, xa), top), zfwd_l=move(x_left, (far, xr), (far, xa), low),
            )
        return moves

    def down_moves(e):
        top, low = pl.ds(0, FF // 2), pl.ds(FF // 2, FF // 2)

        def move(device, src, dst, rows=None):
            if rows is None:
                return Move(wd.at[e, src], wd.at[e, dst], device)
            return Move(wd.at[e, src, rows], wd.at[e, dst, rows], device)

        return dict(
            right=move(x_right, 0, 1), left=move(x_left, 0, 3), z=move(z_far, 0, 4),
            fwd_r=move(x_right, 1, 2, top), fwd_l=move(x_left, 3, 2, low),
            zright=move(x_right, 4, 5), zleft=move(x_left, 4, 7),
            zfwd_r=move(x_right, 5, 6, top), zfwd_l=move(x_left, 7, 6, low),
        )

    gu = [gate_up_moves(e, n, p in X_FIRST) for p, (e, n) in enumerate(PIECES)]
    dn = [down_moves(0), down_moves(1)]

    mine = zh * 4 + x
    loads = {}

    def load(name, src, dst):
        loads[name] = pltpu.make_async_copy(src, dst, local_sem.at[len(loads)])
        loads[name].start()

    order = X_FIRST + Z_FIRST
    for p in order[:2]:
        e, n = PIECES[p]
        load((p, 0), wgu.at[e, :, pl.ds(n * COL, COL)], wg.at[e, n, mine, :, pl.ds(0, COL)])
        load((p, 1), wgu.at[e, :, pl.ds(FF + n * COL, COL)], wg.at[e, n, mine, :, pl.ds(COL, COL)])
    load("tok", tok, tokb.at[OWN, pl.ds(0, TOK)])
    for p in order[2:]:
        e, n = PIECES[p]
        load((p, 0), wgu.at[e, :, pl.ds(n * COL, COL)], wg.at[e, n, mine, :, pl.ds(0, COL)])
        load((p, 1), wgu.at[e, :, pl.ds(FF + n * COL, COL)], wg.at[e, n, mine, :, pl.ds(COL, COL)])
    load("down0", wdn.at[0], wd.at[0, 0])
    load("down1", wdn.at[1], wd.at[1, 0])

    barrier = pltpu.get_barrier_semaphore()
    for peer in (x_right, x_left, z_far, y_right, y_left, z_near, twin):
        pl.semaphore_signal(barrier, inc=1, device_id=peer, device_id_type=MESH)

    weights = probs[...] / jnp.sum(probs[...], axis=0, keepdims=True)
    high = weights.astype(BF16)
    middle = (weights - high.astype(F32)).astype(BF16)
    low = (weights - high.astype(F32) - middle.astype(F32)).astype(BF16)
    numbers = ids[...].astype(F32).astype(BF16)
    for k in range(TOP):
        parts = [v[k : k + 1, :] for v in (numbers, high, middle, low)]
        rows = jnp.concatenate([*parts, jnp.zeros((META - 4, TOK), BF16)], axis=0)
        tokb[OWN, TOK:ROWS, k * TOK : (k + 1) * TOK] = rows

    before = lax.broadcasted_iota(jnp.int32, (TOK, TOK), 0)
    after = lax.broadcasted_iota(jnp.int32, (TOK, TOK), 1)
    tri[...] = jnp.where(before < after, 1.0, 0.0).astype(BF16)
    pl.semaphore_wait(barrier, 7)

    slot_number = lax.broadcasted_iota(jnp.int32, (CAP, TOK), 0).astype(F32)

    def dispatch(r, carry):
        routing = tokb[r, pl.ds(TOK, META), :].astype(F32)
        places, shares = [], []
        for e in range(2):
            number = (ex * 2 + e).astype(F32)
            named = jnp.zeros((1, TOK), F32)
            weight = jnp.zeros((1, TOK), F32)
            for k in range(TOP):
                cols = slice(k * TOK, (k + 1) * TOK)
                hit = routing[0:1, cols] == number
                value = routing[1:2, cols] + routing[2:3, cols] + routing[3:4, cols]
                named = named + jnp.where(hit, 1.0, 0.0)
                weight = weight + jnp.where(hit, value, 0.0)
            many = jnp.broadcast_to(named, (16, TOK)).astype(BF16)
            slot = jnp.dot(many, tri[...], preferred_element_type=F32)[0:1, :]
            place = jnp.where(slot_number == slot, jnp.broadcast_to(named, (CAP, TOK)), 0.0)
            places.append(place)
            shares.append(place * weight)
        share = jnp.concatenate(shares, axis=0).T
        upper = share.astype(BF16)
        pt[0, r, :, :] = upper
        pt[1, r, :, :] = (share - upper.astype(F32)).astype(BF16)
        place = jnp.concatenate(places, axis=0).astype(BF16)
        rows = pl.ds(pl.multiple_of(r * CAP, CAP), CAP)
        for c in range(4):
            cols = slice(c * 512, (c + 1) * 512)
            picked = jnp.dot(place, tokb[r, 0:TOK, cols], preferred_element_type=F32).astype(BF16)
            xs[0, rows, cols] = picked[0:CAP]
            xs[1, rows, cols] = picked[CAP:]
        return carry

    def gate_up(p):
        e, n = PIECES[p]

        def tile(i, carry):
            rows = pl.ds(pl.multiple_of(i * 640, 640), 640)
            both = jnp.dot(xs[e, rows, :], wg[e, n].reshape(D, 2 * COL), preferred_element_type=F32)
            gate, up = both[:, :COL], both[:, COL:]
            hid[e, rows, n * COL : (n + 1) * COL] = (gate / (1.0 + jnp.exp(-gate)) * up).astype(BF16)
            return carry

        lax.fori_loop(0, 2, tile, 0)

    def own_piece(p):
        loads[(p, 0)].wait()
        loads[(p, 1)].wait()
        start(gu[p]["right"], gu[p]["left"])

    def forward(p):
        wait(gu[p]["right"], gu[p]["left"])
        start(gu[p]["fwd_r"], gu[p]["fwd_l"])

    def far_forward(p):
        wait(gu[p]["zright"], gu[p]["zleft"])
        start(gu[p]["zfwd_r"], gu[p]["zfwd_l"])

    def far_start(p):
        wait(gu[p]["z"])
        start(gu[p]["zright"], gu[p]["zleft"])

    own_piece(4)
    loads["tok"].wait()
    start(t_z, t_right, t_left, twins[OWN])
    own_piece(5)
    for p in Z_FIRST:
        own_piece(p)
    start(gu[0]["z"], gu[1]["z"], gu[4]["z"], gu[5]["z"], gu[2]["z"])

    forward(4)
    forward(5)
    start(gu[4]["zl"], gu[5]["zl"], gu[3]["z"], gu[4]["zr"], gu[5]["zr"])
    forward(0)
    wait(t_right)
    start(t_fwd_r)
    wait(t_left)
    start(t_fwd_l)
    wait(t_z)
    start(t_zright, t_zleft, twins[ZED], twins[LEFT], twins[RIGHT])
    forward(1)
    forward(2)
    far_start(0)
    forward(3)
    for s in (OWN, ZED, LEFT, RIGHT):
        wait(twins[s])
    lax.fori_loop(0, 8, dispatch, 0)
    far_start(1)
    wait(t_fwd_r, t_fwd_l)
    start(twins[ACROSS])
    for p in X_FIRST:
        wait(gu[p]["fwd_r"], gu[p]["fwd_l"])
        start(gu[p]["za"])
    far_start(2)
    far_forward(0)
    wait(t_zright)
    start(t_zfwd_r)
    wait(t_zleft)
    start(t_zfwd_l, twins[ZLEFT], twins[ZRIGHT])
    far_forward(1)
    far_start(3)
    for s in (ACROSS, ZLEFT, ZRIGHT):
        wait(twins[s])
    lax.fori_loop(8, 14, dispatch, 0)
    far_forward(2)
    wait(t_zfwd_r, t_zfwd_l)
    start(twins[ZACROSS])
    wait(twins[ZACROSS])
    lax.fori_loop(14, SRC, dispatch, 0)
    for m in token_moves:
        m.wait_send()
    for peer in (y_right, y_left, z_near, twin):
        pl.semaphore_signal(free_sem, inc=1, device_id=peer, device_id_type=MESH)
    loads["down0"].wait()
    loads["down1"].wait()
    start(dn[0]["z"], dn[1]["z"])
    for name in ("fwd_r", "fwd_l", "zfwd_r", "zfwd_l"):
        wait(gu[0][name])
    gate_up(0)
    far_forward(3)
    start(dn[0]["right"], dn[0]["left"], dn[1]["right"], dn[1]["left"])
    for p in (1, 2, 3):
        for name in ("fwd_r", "fwd_l", "zfwd_r", "zfwd_l"):
            wait(gu[p][name])
        gate_up(p)
    for p in X_FIRST:
        for name in ("z", "zl", "zr", "za"):
            wait(gu[p][name])
        gate_up(p)
    pl.semaphore_wait(free_sem, 4)

    def is_z_first(c):
        return (c % 2 == 1) & (c < 6)

    def rows_at(c, first=0, rows=TOK):
        return pl.ds(pl.multiple_of((c % 4) * TOK + first, TOK // 2), rows)

    def theirs_at(c):
        return pl.ds(pl.multiple_of((c % 2) * TOK, TOK), TOK)

    upper, lower = pl.ds(0, TOK // 2), pl.ds(TOK // 2, TOK // 2)
    every = pl.ds(0, TOK)

    def lane(c, width):
        return pl.ds(pl.multiple_of((c % 4) * 512, 512), width)

    class Return:
        def __init__(self, c, z_first=False):
            width = COL if z_first else 2 * COL
            hop_src = [
                (xs.at[0, rows_at(c, 0, TOK // 2), pl.ds(2 * width, width)], y_right),
                (xs.at[0, rows_at(c, TOK // 2, TOK // 2), pl.ds(2 * width, width)], y_left),
                (xs.at[0, rows_at(c), pl.ds(width, width)], y_right),
                (xs.at[0, rows_at(c), pl.ds(3 * width, width)], y_left),
            ]
            hop_dst = [
                tokb.at[8 + c // 4, upper, lane(c, width)],
                tokb.at[8 + c // 4, lower, lane(c, width)],
                tokb.at[10 + c // 4, every, lane(c, width)],
                tokb.at[12 + c // 4, every, lane(c, width)],
            ]
            if z_first:
                z = (xs.at[0, rows_at(c), pl.ds(4 * COL, 4 * COL)], zbuf.at[c // 2], z_near)
            else:
                lands = tokb.at[14, every, pl.ds(pl.multiple_of(c * COL, COL), COL)]
                z = (xs.at[0, rows_at(c), pl.ds(COL, COL)], lands, z_near)
            self.moves = [
                (xs.at[1, theirs_at(c)], tokb.at[c, every], twin),
                *((src, dst, device) for (src, device), dst in zip(hop_src, hop_dst)),
                z,
            ]
            self.c, self.width = c, width

        def copy(self, k):
            src, dst, device = self.moves[k]
            return pltpu.make_async_remote_copy(
                src_ref=src, dst_ref=dst, send_sem=ret_send.at[k, self.c], recv_sem=ret_recv.at[k, self.c],
                device_id=device, device_id_type=MESH,
            )

        def start(self, *which):
            for k in which:
                self.copy(k).start()

        def wait(self, *which):
            for k in which:
                self.copy(k).wait_recv()

        def drain(self, *which):
            for k in which:
                self.copy(k).wait_send()

        def landed(self, k):
            return self.moves[k][1][...]

    def add(rows, cols, *more):
        total = xs[0, rows, cols].astype(F32)
        for m in more:
            total = total + m.astype(F32)
        return total

    def finish(c, total):
        column = ((zh + c // 4) % 2) * 4 + (x + 4 - c % 4) % 4
        out[:, pl.ds(pl.multiple_of(column * COL, COL), COL)] = total.astype(BF16)

    def stage_compute(c):
        @pl.when(c >= 2)
        def _():
            Return(c - 2).drain(0)

        for e in range(2):
            y_e = jnp.dot(hid[e], wd[e, c], preferred_element_type=F32).astype(BF16)
            yb[:, e * CAP : (e + 1) * CAP, :] = y_e.reshape(SRC, CAP, COL)
        kind = is_z_first(c).astype(jnp.int32)

        combine_into(c, kind, 1)
        Return(c).start(0)
        combine_into(c, kind, 0)

    def combine_into(c, kind, parity):
        for (yy, zz), s in RETURN.items():
            place = kind * (4 * zz + yy) + (1 - kind) * (2 * yy + zz)
            cols = pl.ds(pl.multiple_of(place * COL, COL), COL)
            r = s + parity
            total = jnp.dot(pt[0, r], yb[r], preferred_element_type=F32)
            total = total + jnp.dot(pt[1, r], yb[r], preferred_element_type=F32)
            if parity:
                xs[1, theirs_at(c), cols] = total.astype(BF16)
            else:
                xs[0, rows_at(c), cols] = total.astype(BF16)

    def stage_twin(c):
        Return(c).wait(0)

        def rows_of(i, carry):
            rows = pl.ds(pl.multiple_of((c % 4) * TOK + i * 32, 32), 32)
            got = tokb[c, pl.ds(pl.multiple_of(i * 32, 32), 32), :]
            xs[0, rows, :] = add(rows, slice(None), got).astype(BF16)
            return carry

        lax.fori_loop(0, TOK // 32, rows_of, 0)

        @pl.when(is_z_first(c))
        def _():
            Return(c, True).start(5)

        @pl.when(jnp.logical_not(is_z_first(c)))
        def _():
            Return(c).start(1, 2)

    def second_hop(move):
        c, width = move.c, move.width
        move.wait(1)
        rows, cols = rows_at(c, 0, TOK // 2), slice(width, 2 * width)
        xs[0, rows, cols] = add(rows, cols, move.landed(1)).astype(BF16)
        move.start(3)
        move.wait(2)
        rows, cols = rows_at(c, TOK // 2, TOK // 2), slice(3 * width, 4 * width)
        xs[0, rows, cols] = add(rows, cols, move.landed(2)).astype(BF16)
        move.start(4)

    def stage_second(c):
        @pl.when(is_z_first(c))
        def _():
            move = Return(c, True)
            move.wait(5)

            def rows_of(i, carry):
                rows = pl.ds(pl.multiple_of((c % 4) * TOK + i * 32, 32), 32)
                got = zbuf[c // 2, pl.ds(pl.multiple_of(i * 32, 32), 32), :]
                xs[0, rows, 0 : 4 * COL] = add(rows, slice(0, 4 * COL), got).astype(BF16)
                return carry

            lax.fori_loop(0, TOK // 32, rows_of, 0)
            move.start(1, 2)

        @pl.when(jnp.logical_not(is_z_first(c)))
        def _():
            second_hop(Return(c))

    def stage_third(c):
        @pl.when(is_z_first(c))
        def _():
            second_hop(Return(c, True))

        @pl.when(jnp.logical_not(is_z_first(c)))
        def _():
            move = Return(c)
            move.wait(3, 4)
            cols = slice(0, 2 * COL)
            total = add(rows_at(c), cols, move.landed(3), move.landed(4))
            xs[0, rows_at(c), cols] = total.astype(BF16)
            move.start(5)

    def stage_last(c):
        @pl.when(is_z_first(c))
        def _():
            move = Return(c, True)
            move.wait(3, 4)
            finish(c, add(rows_at(c), slice(0, COL), move.landed(3), move.landed(4)))
            move.drain(1, 2, 3, 4, 5)

        @pl.when(jnp.logical_not(is_z_first(c)))
        def _():
            move = Return(c)
            move.wait(5)
            finish(c, add(rows_at(c), slice(0, COL), move.landed(5)))
            move.drain(1, 2, 3, 4, 5)

    def step(i, carry):
        @pl.when(i == 1)
        def _():
            for e in range(2):
                wait(dn[e]["right"], dn[e]["left"])
                start(dn[e]["fwd_r"], dn[e]["fwd_l"])

        @pl.when(i == 2)
        def _():
            for e in range(2):
                wait(dn[e]["z"])
                start(dn[e]["zright"], dn[e]["zleft"])
            for e in range(2):
                wait(dn[e]["fwd_r"], dn[e]["fwd_l"])

        @pl.when(i == 5)
        def _():
            for e in range(2):
                wait(dn[e]["zright"], dn[e]["zleft"])
                start(dn[e]["zfwd_r"], dn[e]["zfwd_l"])

        @pl.when(i == 6)
        def _():
            for e in range(2):
                wait(dn[e]["zfwd_r"], dn[e]["zfwd_l"])

        @pl.when(i < STEPS)
        def _():
            stage_compute(i)

        @pl.when(i < STEPS)
        def _():
            stage_twin(i)

        @pl.when((i >= 1) & (i < STEPS + 1))
        def _():
            stage_second(i - 1)

        @pl.when((i >= 2) & (i < STEPS + 2))
        def _():
            stage_third(i - 2)

        @pl.when(i >= 3)
        def _():
            stage_last(i - 3)

        return carry

    lax.fori_loop(0, STEPS + 3, step, 0)
    Return(STEPS - 2).drain(0)
    Return(STEPS - 1).drain(0)
    for group in (*gu, *dn):
        for m in group.values():
            m.wait_send()


def shards(tokens, expert_ids, route_probs, w_gate_up, w_down):
    any_spec = pl.BlockSpec(memory_space=pl.ANY)
    vmem_spec = pl.BlockSpec(memory_space=pltpu.VMEM)
    return pl.pallas_call(
        kernel,
        out_shape=jax.ShapeDtypeStruct((TOK, D), BF16),
        in_specs=[any_spec, vmem_spec, vmem_spec, any_spec, any_spec],
        out_specs=vmem_spec,
        scratch_shapes=[
            pltpu.VMEM((SRC, ROWS, D), BF16),
            pltpu.VMEM((2, 3, STEPS, COL, 2 * COL), BF16),
            pltpu.VMEM((2, STEPS, FF, COL), BF16),
            pltpu.VMEM((2, SRC * CAP, D), BF16),
            pltpu.VMEM((2, SRC * CAP, FF), BF16),
            pltpu.VMEM((2, SRC, TOK, 2 * CAP), BF16),
            pltpu.VMEM((SRC, 2 * CAP, COL), BF16),
            pltpu.VMEM((TOK, TOK), BF16),
            pltpu.VMEM((3, TOK, 4 * COL), BF16),
            pltpu.SemaphoreType.DMA((15,)),
            pltpu.SemaphoreType.DMA((MOVES,)),
            pltpu.SemaphoreType.DMA((MOVES,)),
            pltpu.SemaphoreType.DMA((6, STEPS)),
            pltpu.SemaphoreType.DMA((6, STEPS)),
            pltpu.SemaphoreType.REGULAR,
        ],
        compiler_params=pltpu.CompilerParams(
            collective_id=0, has_side_effects=True, vmem_limit_bytes=67_000_000
        ),
    )(tokens, expert_ids.T, route_probs.T, w_gate_up, w_down)


def solution(mesh):
    spec = P(("dp", "expert"), None)
    in_specs = (spec, spec, spec, P("expert", "dp", None), P("expert", None, "dp"))
    return jax.shard_map(shards, mesh=mesh, in_specs=in_specs, out_specs=spec, check_vma=False)
```

```python
import jax
import jax.numpy as jnp
from jax import lax
from jax.experimental import pallas as pl
from jax.experimental.pallas import tpu as pltpu
from jax.sharding import PartitionSpec as P

MESH = pl.DeviceIdType.MESH
F32 = jnp.float32
BF16 = jnp.bfloat16

TOK = 256
META = 16
ROWS = TOK + META
HALF = 144
D = 2048
FF = 768
TOP = 8
CAP = 80
SRC = 16
COL = 256
STEPS = 8
MOVES = 17 + 4 * 9 + 8 + 9 + 2 * 9

OWN, ZED, LEFT, RIGHT, ACROSS, ZLEFT, ZRIGHT, ZACROSS = range(0, 16, 2)
RETURN = {
    (0, 0): OWN, (0, 1): ZED, (1, 0): RIGHT, (1, 1): ZRIGHT,
    (2, 0): ACROSS, (2, 1): ZACROSS, (3, 0): LEFT, (3, 1): ZLEFT,
}
PIECES = [(e, n) for e in range(2) for n in range(3)]
Z_FIRST = (0, 1, 2, 3)
X_FIRST = (4, 5)
Z_ACROSS = 4

DOWN = (0, 1, 3, 4, 2, 5, 7, 6)
RETURN_Z_FIRST = (1, 4, 6)
PLAN = (
    ("n", 0), ("C", 0), ("T", 0), ("n", 1), ("f", 0), ("C", 1), ("S", 0), ("T", 1), ("C", 2), ("f", 1),
    ("C", 3), ("T", 2), ("T", 3), ("H", 0), ("a", 0), ("a", 1), ("C", 4), ("S", 2), ("T", 4), ("S", 1),
    ("F", 0), ("S", 3), ("L", 0), ("H", 2), ("H", 1), ("F", 1), ("C", 5), ("C", 6), ("T", 5), ("S", 4), ("T", 6),
    ("H", 3), ("S", 5), ("L", 2), ("L", 1), ("A", 0), ("A", 1), ("H", 4), ("C", 7), ("T", 7), ("H", 5), ("S", 6), ("S", 7),
    ("H", 6), ("L", 4), ("L", 3), ("L", 5), ("H", 7), ("L", 6), ("L", 7),
)


def kernel(
    tok, ids, probs, wgu, wdn, out,
    tokb, wg, wd, xs, hid, pt, yb, tri, zbuf,
    local_sem, send_sem, recv_sem, ret_send, ret_recv, free_sem,
):
    dp, ex = lax.axis_index("dp"), lax.axis_index("expert")
    zh, x = dp // 4, dp % 4
    y, zl, core = ex // 4, (ex // 2) % 2, ex % 2
    xl, xr, xa = (x + 3) % 4, (x + 1) % 4, (x + 2) % 4

    def at_dp(zhi, xx):
        return (zhi * 4 + xx, ex)

    def at_ex(yy, zz, cc):
        return (dp, (yy * 2 + zz) * 2 + cc)

    x_right, x_left, z_far = at_dp(zh, xr), at_dp(zh, xl), at_dp(1 - zh, x)
    y_right, y_left = at_ex((y + 1) % 4, zl, core), at_ex((y + 3) % 4, zl, core)
    z_near, twin = at_ex(y, 1 - zl, core), at_ex(y, zl, 1 - core)

    count = [0]

    class Move:
        def __init__(self, src, dst, device, lands=None):
            n = count[0]
            count[0] += 1
            sems = dict(send_sem=send_sem.at[n], recv_sem=recv_sem.at[n], device_id=device, device_id_type=MESH)
            lands = dst if lands is None else lands
            self.out = lambda: pltpu.make_async_remote_copy(src_ref=src, dst_ref=dst, **sems)
            self.into = lambda: pltpu.make_async_remote_copy(src_ref=lands, dst_ref=lands, **sems)

        def start(self):
            self.out().start()

        def wait_send(self):
            self.out().wait_send()

        def wait_recv(self):
            self.into().wait_recv()

    def start(*moves):
        for m in moves:
            m.start()

    def wait(*moves):
        for m in moves:
            m.wait_recv()

    first, second = pl.ds(0, HALF), pl.ds(HALF, ROWS - HALF)

    def block(src, dst, device, rows=None):
        if rows is None:
            return Move(tokb.at[src], tokb.at[dst], device)
        return Move(tokb.at[src, rows], tokb.at[dst, rows], device)

    t_z = block(OWN, ZED, z_near)
    t_right, t_left = block(OWN, LEFT, y_right), block(OWN, RIGHT, y_left)
    t_fwd_r, t_fwd_l = block(LEFT, ACROSS, y_right, first), block(RIGHT, ACROSS, y_left, second)
    t_zright, t_zleft = block(ZED, ZLEFT, y_right), block(ZED, ZRIGHT, y_left)
    t_zfwd_r, t_zfwd_l = block(ZLEFT, ZACROSS, y_right, first), block(ZRIGHT, ZACROSS, y_left, second)
    twins = {s: block(s, s + 1, twin) for s in range(0, SRC, 2)}
    token_moves = [t_z, t_right, t_left, t_fwd_r, t_fwd_l, t_zright, t_zleft, t_zfwd_r, t_zfwd_l, *twins.values()]

    def gate_up_moves(e, n, x_first, z_across):
        def move(device, sends, takes, rows=None):
            src, lands = wg.at[e, n, sends[0] * 4 + sends[1]], wg.at[e, n, takes[0] * 4 + takes[1]]
            if rows is not None:
                src, lands = src.at[rows], lands.at[rows]
            return Move(src, src, device, lands)

        top, low = pl.ds(0, COL // 2), pl.ds(COL // 2, COL // 2)
        far = 1 - zh
        moves = dict(
            right=move(x_right, (zh, x), (zh, xl)), left=move(x_left, (zh, x), (zh, xr)),
            fwd_r=move(x_right, (zh, xl), (zh, xa), top), fwd_l=move(x_left, (zh, xr), (zh, xa), low),
            z=move(z_far, (zh, x), (far, x)),
        )
        if x_first:
            moves.update(
                zl=move(z_far, (zh, xl), (far, xl)), zr=move(z_far, (zh, xr), (far, xr)),
            )
        else:
            moves.update(
                zright=move(x_right, (far, x), (far, xl)), zleft=move(x_left, (far, x), (far, xr)),
            )
        if z_across:
            moves.update(za=move(z_far, (zh, xa), (far, xa)))
        else:
            moves.update(
                zfwd_r=move(x_right, (far, xl), (far, xa), top), zfwd_l=move(x_left, (far, xr), (far, xa), low),
            )
        return moves

    def down_moves(e):
        top, low = pl.ds(0, FF // 2), pl.ds(FF // 2, FF // 2)

        def move(device, src, dst, rows=None):
            if rows is None:
                return Move(wd.at[e, src], wd.at[e, dst], device)
            return Move(wd.at[e, src, rows], wd.at[e, dst, rows], device)

        return dict(
            right=move(x_right, 0, 1), left=move(x_left, 0, 3), z=move(z_far, 0, 4),
            fwd_r=move(x_right, 1, 2, top), fwd_l=move(x_left, 3, 2, low),
            zright=move(x_right, 4, 5), zleft=move(x_left, 4, 7),
            zfwd_r=move(x_right, 5, 6, top), zfwd_l=move(x_left, 7, 6, low),
        )

    gu = [gate_up_moves(e, n, p in X_FIRST, p == Z_ACROSS) for p, (e, n) in enumerate(PIECES)]
    dn = [down_moves(0), down_moves(1)]

    mine = zh * 4 + x
    loads = {}

    def load(name, src, dst):
        loads[name] = pltpu.make_async_copy(src, dst, local_sem.at[len(loads)])
        loads[name].start()

    order = X_FIRST + Z_FIRST
    for p in order[:2]:
        e, n = PIECES[p]
        load((p, 0), wgu.at[e, :, pl.ds(n * COL, COL)], wg.at[e, n, mine, :, pl.ds(0, COL)])
        load((p, 1), wgu.at[e, :, pl.ds(FF + n * COL, COL)], wg.at[e, n, mine, :, pl.ds(COL, COL)])
    load("tok", tok, tokb.at[OWN, pl.ds(0, TOK)])
    for p in order[2:]:
        e, n = PIECES[p]
        load((p, 0), wgu.at[e, :, pl.ds(n * COL, COL)], wg.at[e, n, mine, :, pl.ds(0, COL)])
        load((p, 1), wgu.at[e, :, pl.ds(FF + n * COL, COL)], wg.at[e, n, mine, :, pl.ds(COL, COL)])
    load("down0", wdn.at[0], wd.at[0, 0])
    load("down1", wdn.at[1], wd.at[1, 0])

    barrier = pltpu.get_barrier_semaphore()
    for peer in (x_right, x_left, z_far, y_right, y_left, z_near, twin):
        pl.semaphore_signal(barrier, inc=1, device_id=peer, device_id_type=MESH)

    weights = probs[...] / jnp.sum(probs[...], axis=0, keepdims=True)
    high = weights.astype(BF16)
    middle = (weights - high.astype(F32)).astype(BF16)
    low = (weights - high.astype(F32) - middle.astype(F32)).astype(BF16)
    numbers = ids[...].astype(F32).astype(BF16)
    for k in range(TOP):
        parts = [v[k : k + 1, :] for v in (numbers, high, middle, low)]
        rows = jnp.concatenate([*parts, jnp.zeros((META - 4, TOK), BF16)], axis=0)
        tokb[OWN, TOK:ROWS, k * TOK : (k + 1) * TOK] = rows

    before = lax.broadcasted_iota(jnp.int32, (TOK, TOK), 0)
    after = lax.broadcasted_iota(jnp.int32, (TOK, TOK), 1)
    tri[...] = jnp.where(before < after, 1.0, 0.0).astype(BF16)
    pl.semaphore_wait(barrier, 7)

    slot_number = lax.broadcasted_iota(jnp.int32, (CAP, TOK), 0).astype(F32)

    def dispatch(r, carry):
        routing = tokb[r, pl.ds(TOK, META), :].astype(F32)
        places, shares = [], []
        for e in range(2):
            number = (ex * 2 + e).astype(F32)
            named = jnp.zeros((1, TOK), F32)
            weight = jnp.zeros((1, TOK), F32)
            for k in range(TOP):
                cols = slice(k * TOK, (k + 1) * TOK)
                hit = routing[0:1, cols] == number
                value = routing[1:2, cols] + routing[2:3, cols] + routing[3:4, cols]
                named = named + jnp.where(hit, 1.0, 0.0)
                weight = weight + jnp.where(hit, value, 0.0)
            many = jnp.broadcast_to(named, (16, TOK)).astype(BF16)
            slot = jnp.dot(many, tri[...], preferred_element_type=F32)[0:1, :]
            place = jnp.where(slot_number == slot, jnp.broadcast_to(named, (CAP, TOK)), 0.0)
            places.append(place)
            shares.append(place * weight)
        share = jnp.concatenate(shares, axis=0).T
        upper = share.astype(BF16)
        pt[0, r, :, :] = upper
        pt[1, r, :, :] = (share - upper.astype(F32)).astype(BF16)
        place = jnp.concatenate(places, axis=0).astype(BF16)
        rows = pl.ds(pl.multiple_of(r * CAP, CAP), CAP)
        for c in range(4):
            cols = slice(c * 512, (c + 1) * 512)
            picked = jnp.dot(place, tokb[r, 0:TOK, cols], preferred_element_type=F32).astype(BF16)
            xs[0, rows, cols] = picked[0:CAP]
            xs[1, rows, cols] = picked[CAP:]
        return carry

    def gate_up(p, *halves):
        e, n = PIECES[p]

        def tile(i, carry):
            rows = pl.ds(pl.multiple_of(i * 640, 640), 640)
            both = jnp.dot(xs[e, rows, :], wg[e, n].reshape(D, 2 * COL), preferred_element_type=F32)
            gate, up = both[:, :COL], both[:, COL:]
            hid[e, rows, n * COL : (n + 1) * COL] = (gate / (1.0 + jnp.exp(-gate)) * up).astype(BF16)
            return carry

        lax.fori_loop(halves[0], halves[-1] + 1, tile, 0)

    def own_piece(p):
        loads[(p, 0)].wait()
        loads[(p, 1)].wait()
        start(gu[p]["right"], gu[p]["left"])

    def forward(p):
        wait(gu[p]["right"], gu[p]["left"])
        start(gu[p]["fwd_r"], gu[p]["fwd_l"])

    def far_forward(p):
        wait(gu[p]["zright"], gu[p]["zleft"])
        start(gu[p]["zfwd_r"], gu[p]["zfwd_l"])

    def far_start(p):
        wait(gu[p]["z"])
        start(gu[p]["zright"], gu[p]["zleft"])

    def whole_piece(p):
        names = [k for k in gu[p] if k.startswith(("fwd", "zfwd", "za"))]
        if p in X_FIRST:
            names = [k for k in names if not k.startswith("fwd")] + ["z"] + (["zl", "zr"] if p == Z_ACROSS else [])
        wait(*(gu[p][k] for k in names))

    own_piece(4)
    loads["tok"].wait()
    start(t_z, t_right, t_left, twins[OWN])
    own_piece(5)
    for p in Z_FIRST:
        own_piece(p)
    start(gu[0]["z"], gu[1]["z"], gu[4]["z"], gu[5]["z"], gu[2]["z"])

    forward(4)
    forward(5)
    start(gu[4]["zl"], gu[5]["zl"], gu[3]["z"], gu[4]["zr"], gu[5]["zr"])
    forward(0)
    wait(t_right)
    start(t_fwd_r)
    wait(t_left)
    start(t_fwd_l)
    wait(t_z)
    start(t_zright, t_zleft, twins[ZED], twins[LEFT], twins[RIGHT])
    forward(1)
    forward(2)
    far_start(0)
    forward(3)
    for s in (OWN, ZED, LEFT, RIGHT):
        wait(twins[s])
    lax.fori_loop(0, 8, dispatch, 0)
    far_start(1)
    wait(t_fwd_r, t_fwd_l)
    start(twins[ACROSS])
    for p in X_FIRST:
        wait(gu[p]["fwd_r"], gu[p]["fwd_l"])
        if p == Z_ACROSS:
            start(gu[p]["za"])
    far_start(2)
    far_forward(0)
    wait(t_zright)
    start(t_zfwd_r)
    wait(t_zleft)
    start(t_zfwd_l, twins[ZLEFT], twins[ZRIGHT])
    far_forward(1)
    whole_piece(0)
    gate_up(0, 0)
    far_start(3)
    for s in (ACROSS, ZLEFT, ZRIGHT):
        wait(twins[s])
    lax.fori_loop(8, 14, dispatch, 0)
    far_forward(2)
    wait(t_zfwd_r, t_zfwd_l)
    start(twins[ZACROSS])
    whole_piece(1)
    gate_up(1, 0)
    wait(twins[ZACROSS])
    lax.fori_loop(14, SRC, dispatch, 0)
    gate_up(0, 1)
    for m in token_moves:
        m.wait_send()
    for peer in (y_right, y_left, z_near, twin):
        pl.semaphore_signal(free_sem, inc=1, device_id=peer, device_id_type=MESH)
    loads["down0"].wait()
    loads["down1"].wait()
    start(dn[0]["z"], dn[1]["z"])
    gate_up(1, 1)
    far_forward(3)
    whole_piece(2)
    gate_up(2, 0, 1)
    wait(gu[5]["zl"], gu[5]["zr"])
    start(gu[5]["zfwd_r"], gu[5]["zfwd_l"])
    start(dn[0]["right"], dn[0]["left"], dn[1]["right"], dn[1]["left"])
    for p in (3, 4, 5):
        whole_piece(p)
        gate_up(p, 0, 1)
    pl.semaphore_wait(free_sem, 4)

    def own_rows(c, first=0, rows=TOK):
        e, at = (0, c) if c < 5 else (1, c - 3)
        return e, pl.ds(at * TOK + first, rows)

    upper, lower = pl.ds(0, TOK // 2), pl.ds(TOK // 2, TOK // 2)
    every = pl.ds(0, TOK)

    class Return:
        def __init__(self, c):
            self.c, self.z_first = c, c in RETURN_Z_FIRST
            self.width = width = COL if self.z_first else 2 * COL
            lane = pl.ds(c % 4 * 512, width)

            def mine(col, cols, first=0, rows=TOK):
                e, at = own_rows(c, first, rows)
                return xs.at[e, at, pl.ds(col, cols)]

            if self.z_first:
                z = (mine(4 * COL, 4 * COL), zbuf.at[RETURN_Z_FIRST.index(c)], z_near)
            else:
                z = (mine(COL, COL), tokb.at[14, every, pl.ds(c * COL, COL)], z_near)
            half = TOK // 2
            self.moves = dict(
                twin=(xs.at[1, pl.ds(c % 2 * TOK, TOK)], tokb.at[c, every], twin),
                right1=(mine(2 * width, width, 0, half), tokb.at[8 + c // 4, upper, lane], y_right),
                left1=(mine(2 * width, width, half, half), tokb.at[8 + c // 4, lower, lane], y_left),
                right2=(mine(width, width), tokb.at[10 + c // 4, every, lane], y_right),
                left2=(mine(3 * width, width), tokb.at[12 + c // 4, every, lane], y_left),
                z=z,
            )
            self.names = list(self.moves)

        def copy(self, name):
            (src, dst, device), k = self.moves[name], self.names.index(name)
            return pltpu.make_async_remote_copy(
                src_ref=src, dst_ref=dst, send_sem=ret_send.at[k, self.c], recv_sem=ret_recv.at[k, self.c],
                device_id=device, device_id_type=MESH,
            )

        def start(self, *names):
            for name in names:
                self.copy(name).start()

        def wait_recv(self, *names):
            for name in names:
                self.copy(name).wait_recv()

        def wait_send(self, *names):
            for name in names:
                self.copy(name).wait_send()

        def landed(self, name):
            return self.moves[name][1][...].astype(F32)

        def place(self, yy, zz):
            return 4 * zz + yy if self.z_first else 2 * yy + zz

        def combine(self, parity):
            for (yy, zz), s in RETURN.items():
                cols = slice(self.place(yy, zz) * COL, (self.place(yy, zz) + 1) * COL)
                r = s + parity
                total = jnp.dot(pt[0, r], yb[r], preferred_element_type=F32)
                total = total + jnp.dot(pt[1, r], yb[r], preferred_element_type=F32)
                if parity:
                    xs[1, pl.ds(self.c % 2 * TOK, TOK), cols] = total.astype(BF16)
                else:
                    e, rows = own_rows(self.c)
                    xs[e, rows, cols] = total.astype(BF16)

        def compute(self):
            if self.c >= 2:
                returns[self.c - 2].wait_send("twin")
            for e in range(2):
                y_e = jnp.dot(hid[e], wd[e, DOWN[self.c]], preferred_element_type=F32).astype(BF16)
                yb[:, e * CAP : (e + 1) * CAP, :] = y_e.reshape(SRC, CAP, COL)
            self.combine(1)
            self.start("twin")
            self.combine(0)

        def add(self, theirs, cols):
            e, rows = own_rows(self.c)

            def some(i, carry):
                at = pl.ds(pl.multiple_of(rows.start + i * 32, 32), 32)
                got = theirs[pl.ds(pl.multiple_of(i * 32, 32), 32), :].astype(F32)
                xs[e, at, 0:cols] = (xs[e, at, 0:cols].astype(F32) + got).astype(BF16)
                return carry

            lax.fori_loop(0, TOK // 32, some, 0)

        def join_twin(self):
            self.wait_recv("twin")
            self.add(tokb.at[self.c], D)
            self.start(*(("z",) if self.z_first else ("right1", "left1")))

        def second(self):
            width, half = self.width, TOK // 2
            for there, col, first in (("right", width, 0), ("left", 3 * width, half)):
                self.wait_recv(there + "1")
                e, rows = own_rows(self.c, first, half)
                total = xs[e, rows, col : col + width].astype(F32) + self.landed(there + "1")
                xs[e, rows, col : col + width] = total.astype(BF16)
                self.start(there + "2")

        def home(self):
            self.wait_recv("right2", "left2")
            e, rows = own_rows(self.c)
            return xs[e, rows, 0 : self.width].astype(F32) + self.landed("right2") + self.landed("left2")

        def hop(self):
            if self.z_first:
                self.wait_recv("z")
                self.add(zbuf.at[RETURN_Z_FIRST.index(self.c)], 4 * COL)
                self.start("right1", "left1")
            else:
                self.second()

        def third(self):
            if self.z_first:
                self.second()
            else:
                total = self.home()
                e, rows = own_rows(self.c)
                xs[e, rows, 0 : self.width] = total.astype(BF16)
                self.start("z")

        def last(self):
            if self.z_first:
                total = self.home()
            else:
                self.wait_recv("z")
                e, rows = own_rows(self.c)
                total = xs[e, rows, 0:COL].astype(F32) + self.landed("z")
            slot = DOWN[self.c]
            column = ((zh + slot // 4) % 2) * 4 + (x + 4 - slot % 4) % 4
            out[:, pl.ds(pl.multiple_of(column * COL, COL), COL)] = total.astype(BF16)

    def down_near(e):
        wait(dn[e]["right"], dn[e]["left"])
        start(dn[e]["fwd_r"], dn[e]["fwd_l"])

    def down_far(e):
        wait(dn[e]["z"])
        start(dn[e]["zright"], dn[e]["zleft"])

    def down_across(e):
        wait(dn[e]["fwd_r"], dn[e]["fwd_l"])

    def down_far_forward(e):
        wait(dn[e]["zright"], dn[e]["zleft"])
        start(dn[e]["zfwd_r"], dn[e]["zfwd_l"])

    def down_far_across(e):
        wait(dn[e]["zfwd_r"], dn[e]["zfwd_l"])

    returns = [Return(c) for c in range(STEPS)]
    do = {
        "C": lambda c: returns[c].compute(), "T": lambda c: returns[c].join_twin(),
        "S": lambda c: returns[c].hop(), "H": lambda c: returns[c].third(), "L": lambda c: returns[c].last(),
        "n": down_near, "f": down_far, "a": down_across, "F": down_far_forward, "A": down_far_across,
    }
    for what, n in PLAN:
        do[what](n)
    for c in range(STEPS):
        returns[c].wait_send(*returns[c].names[0 if c >= STEPS - 2 else 1 :])
    for group in (*gu, *dn):
        for m in group.values():
            m.wait_send()


def shards(tokens, expert_ids, route_probs, w_gate_up, w_down):
    any_spec = pl.BlockSpec(memory_space=pl.ANY)
    vmem_spec = pl.BlockSpec(memory_space=pltpu.VMEM)
    return pl.pallas_call(
        kernel,
        out_shape=jax.ShapeDtypeStruct((TOK, D), BF16),
        in_specs=[any_spec, vmem_spec, vmem_spec, any_spec, any_spec],
        out_specs=vmem_spec,
        scratch_shapes=[
            pltpu.VMEM((SRC, ROWS, D), BF16),
            pltpu.VMEM((2, 3, STEPS, COL, 2 * COL), BF16),
            pltpu.VMEM((2, STEPS, FF, COL), BF16),
            pltpu.VMEM((2, SRC * CAP, D), BF16),
            pltpu.VMEM((2, SRC * CAP, FF), BF16),
            pltpu.VMEM((2, SRC, TOK, 2 * CAP), BF16),
            pltpu.VMEM((SRC, 2 * CAP, COL), BF16),
            pltpu.VMEM((TOK, TOK), BF16),
            pltpu.VMEM((3, TOK, 4 * COL), BF16),
            pltpu.SemaphoreType.DMA((15,)),
            pltpu.SemaphoreType.DMA((MOVES,)),
            pltpu.SemaphoreType.DMA((MOVES,)),
            pltpu.SemaphoreType.DMA((6, STEPS)),
            pltpu.SemaphoreType.DMA((6, STEPS)),
            pltpu.SemaphoreType.REGULAR,
        ],
        compiler_params=pltpu.CompilerParams(
            collective_id=0, has_side_effects=True, vmem_limit_bytes=67_000_000
        ),
    )(tokens, expert_ids.T, route_probs.T, w_gate_up, w_down)


def solution(mesh):
    spec = P(("dp", "expert"), None)
    in_specs = (spec, spec, spec, P("expert", "dp", None), P("expert", None, "dp"))
    return jax.shard_map(shards, mesh=mesh, in_specs=in_specs, out_specs=spec, check_vma=False)
```

```python
import functools

import jax
import jax.numpy as jnp
from jax import lax
from jax.experimental import pallas as pl
from jax.experimental.pallas import tpu as pltpu
from jax.sharding import PartitionSpec as P

MESH = pl.DeviceIdType.MESH
F32 = jnp.float32
BF16 = jnp.bfloat16

TOK = 256
META = 16
ROWS = TOK + META
HALF = 144
D = 2048
FF = 768
TOP = 8
CAP = 80
SRC = 16
COL = 256
SHARDS = 8
STEPS = 16
STEP = COL // 2
LANDINGS = 8 + 4 * 4 + 3 + 4 + 2 * 5 + 16 * 4
SENDS = 1 + 6 + 2 + 1 + 4

OWN, ZED, LEFT, RIGHT, ACROSS, ZLEFT, ZRIGHT, ZACROSS = range(0, 16, 2)
RETURN = {
    (0, 0): OWN, (0, 1): ZED, (1, 0): RIGHT, (1, 1): ZRIGHT,
    (2, 0): ACROSS, (2, 1): ZACROSS, (3, 0): LEFT, (3, 1): ZLEFT,
}
PIECES = [(e, n) for e in range(2) for n in range(3)]
Z_FIRST = (0, 1, 2, 3)
X_FIRST = (4, 5)
Z_ACROSS = 4

UNITS = (
    ((0, 0), (0, 1)), ((1, 0), (3, 0)), ((1, 1), (3, 1)), ((4, 0), (4, 1)), ((2, 0), (2, 1)), ((5, 0), (7, 0)), ((5, 1), (7, 1)), ((6, 0),), ((6, 1),),
)
RETURN_Z_FIRST = (4, 6, 10, 12, 14)
Z_LAST = ()
PLAN = (
    ("C", 0), ("T", 0), ("T", 1), ("S", 0), ("n", 0), ("S", 1), ("C", 1), ("T", 2), ("T", 3), ("H", 1),
    ("n", 1), ("f", 0), ("f", 1), ("S", 2), ("H", 0), ("C", 2), ("C", 3), ("T", 4), ("T", 5), ("S", 3),
    ("T", 6), ("C", 4), ("S", 5), ("T", 9), ("S", 4), ("H", 3), ("T", 8), ("T", 7), ("S", 9), ("C", 5),
    ("S", 8), ("S", 6), ("H", 5), ("F", 0), ("L", 3), ("H", 4), ("T", 10), ("T", 11), ("H", 9), ("S", 7),
    ("F", 1), ("C", 6), ("T", 12), ("S", 11), ("C", 7), ("T", 13), ("S", 10), ("H", 6), ("T", 14), ("C", 8),
    ("T", 15), ("S", 13), ("S", 12), ("H", 11), ("L", 4), ("L", 9), ("S", 15), ("L", 6), ("H", 8), ("S", 14),
    ("H", 13), ("H", 12), ("H", 7), ("H", 10), ("L", 1), ("H", 2), ("L", 11), ("L", 5), ("L", 0), ("H", 15),
    ("H", 14), ("L", 10), ("L", 2), ("L", 12), ("L", 7), ("L", 13), ("L", 8), ("L", 15), ("L", 14),
)


def kernel(
    tok, ids, probs, wgu, wdn, out,
    tokb, wg, wd, xs, hid, pt, yb, tri, zbuf, ob, part,
    local_sem, send_sem, recv_sem, out_sem, free_sem,
):
    dp, ex = lax.axis_index("dp"), lax.axis_index("expert")
    zh, x = dp // 4, dp % 4
    y, zl, core = ex // 4, (ex // 2) % 2, ex % 2
    xl, xr, xa = (x + 3) % 4, (x + 1) % 4, (x + 2) % 4

    def at_dp(zhi, xx):
        return (zhi * 4 + xx, ex)

    def at_ex(yy, zz, cc):
        return (dp, (yy * 2 + zz) * 2 + cc)

    x_right, x_left, z_far = at_dp(zh, xr), at_dp(zh, xl), at_dp(1 - zh, x)
    y_right, y_left = at_ex((y + 1) % 4, zl, core), at_ex((y + 3) % 4, zl, core)
    z_near, twin = at_ex(y, 1 - zl, core), at_ex(y, zl, 1 - core)

    counts = dict(send=0, recv=0)

    def semaphore(kind):
        counts[kind] += 1
        return (send_sem if kind == "send" else recv_sem).at[counts[kind] - 1]

    def described(src, dst, send, recv, device):
        return pltpu.make_async_remote_copy(
            src_ref=src, dst_ref=dst, send_sem=send, recv_sem=recv, device_id=device, device_id_type=MESH
        )

    class Landing:
        def __init__(self, ref):
            self.ref, self.semaphore = ref, semaphore("recv")

        def wait(self):
            described(self.ref, self.ref, all_sent[0], self.semaphore, twin).wait_recv()

    class Sent:
        def __init__(self, ref):
            self.ref, self.semaphore = ref, semaphore("send")
            all_sent.append(self.semaphore)

        def wait(self):
            described(self.ref, self.ref, self.semaphore, recv_sem.at[0], twin).wait_send()

    all_sent = []

    def move(src, dst, device, sent, landing):
        return functools.partial(described, src, dst, sent.semaphore, landing.semaphore, device)

    def start(*moves):
        for m in moves:
            m().start()

    first, second = pl.ds(0, HALF), pl.ds(HALF, ROWS - HALF)

    def blocks(n):
        return tokb.at[pl.ds(0, n)]

    tokens_sent = Sent(blocks(15))
    z_in, near_in, across_in, far_in, last_in = (Landing(blocks(n)) for n in (1, 2, 1, 2, 1))
    twins_in = [Landing(blocks(n)) for n in (4, 3, 1)]

    def block(src, dst, device, landing, rows=slice(None)):
        return move(tokb.at[src, rows], tokb.at[dst, rows], device, tokens_sent, landing)

    t_z = block(OWN, ZED, z_near, z_in)
    t_right, t_left = block(OWN, LEFT, y_right, near_in), block(OWN, RIGHT, y_left, near_in)
    t_fwd_r = block(LEFT, ACROSS, y_right, across_in, first)
    t_fwd_l = block(RIGHT, ACROSS, y_left, across_in, second)
    t_zright, t_zleft = block(ZED, ZLEFT, y_right, far_in), block(ZED, ZRIGHT, y_left, far_in)
    t_zfwd_r = block(ZLEFT, ZACROSS, y_right, last_in, first)
    t_zfwd_l = block(ZRIGHT, ZACROSS, y_left, last_in, second)
    waves = {OWN: 0, ZED: 0, LEFT: 0, RIGHT: 0, ACROSS: 1, ZLEFT: 1, ZRIGHT: 1, ZACROSS: 2}
    twins = {s: block(s, s + 1, twin, twins_in[w]) for s, w in waves.items()}

    class GateUp:
        def __init__(self, p):
            e, n = PIECES[p]
            top, low = pl.ds(0, COL // 2), pl.ds(COL // 2, COL // 2)
            far = 1 - zh

            def shards(k):
                return wg.at[e, n, pl.ds(0, k)]

            self.sent, self.near_in = Sent(shards(7)), Landing(shards(2))
            if p in Z_FIRST:
                self.z_in, self.far_in = Landing(shards(1)), Landing(shards(2))
                self.rest_in = across_in = Landing(shards(2))
                z_in, last_in = self.z_in, self.rest_in
            elif p == Z_ACROSS:
                self.across_in, self.rest_in = Landing(shards(1)), Landing(shards(4))
                across_in = self.across_in
                z_in = self.far_in = last_in = self.rest_in
            else:
                self.across_in, self.far_in = Landing(shards(1)), Landing(shards(2))
                self.rest_in, across_in = Landing(shards(2)), self.across_in
                z_in = last_in = self.rest_in

            def same(device, z, xx, landing, rows=slice(None)):
                ref = wg.at[e, n, z * 4 + xx, rows]
                return move(ref, ref, device, self.sent, landing)

            self.right, self.left = same(x_right, zh, x, self.near_in), same(x_left, zh, x, self.near_in)
            self.fwd_r, self.fwd_l = same(x_right, zh, xl, across_in, top), same(x_left, zh, xr, across_in, low)
            self.z = same(z_far, zh, x, z_in)
            if p in X_FIRST:
                self.zl, self.zr = same(z_far, zh, xl, self.far_in), same(z_far, zh, xr, self.far_in)
            else:
                self.zright, self.zleft = same(x_right, far, x, self.far_in), same(x_left, far, x, self.far_in)
            if p == Z_ACROSS:
                self.za = same(z_far, zh, xa, last_in)
            else:
                self.zfwd_r, self.zfwd_l = same(x_right, far, xl, last_in, top), same(x_left, far, xr, last_in, low)

    class Down:
        def __init__(self, half):
            top, low = pl.ds(0, FF // 2), pl.ds(FF // 2, FF // 2)
            cols = pl.ds(half * STEP, STEP)

            def slots(k):
                return wd.at[pl.ds(0, k), :, :, cols]

            self.sent = Sent(slots(7))
            self.near_in, self.across_in, self.z_in, self.far_in, self.last_in = (
                Landing(slots(k)) for k in (2, 1, 1, 2, 1)
            )

            def to(device, src, dst, landing, rows=slice(None)):
                return move(wd.at[src, :, rows, cols], wd.at[dst, :, rows, cols], device, self.sent, landing)

            self.right, self.left = to(x_right, 0, 1, self.near_in), to(x_left, 0, 3, self.near_in)
            self.z = to(z_far, 0, 4, self.z_in)
            self.fwd_r, self.fwd_l = to(x_right, 1, 2, self.across_in, top), to(x_left, 3, 2, self.across_in, low)
            self.zright, self.zleft = to(x_right, 4, 5, self.far_in), to(x_left, 4, 7, self.far_in)
            if half in Z_LAST:
                self.za = to(z_far, 2, 6, self.last_in)
            else:
                self.zfwd_r, self.zfwd_l = to(x_right, 5, 6, self.last_in, top), to(x_left, 7, 6, self.last_in, low)

    gu = [GateUp(p) for p in range(6)]
    dn = [Down(0), Down(1)]

    mine = zh * 4 + x
    def load(src, dst, name):
        pltpu.make_async_copy(src, dst, local_sem.at[name]).start()

    def loaded(dst, name):
        pltpu.make_async_copy(dst, dst, local_sem.at[name]).wait()

    def load_piece(p):
        e, n = PIECES[p]
        load(wgu.at[e, :, pl.ds(n * COL, COL)], wg.at[e, n, mine, :, pl.ds(0, COL)], p)
        load(wgu.at[e, :, pl.ds(FF + n * COL, COL)], wg.at[e, n, mine, :, pl.ds(COL, COL)], p)

    load_piece(4)
    load_piece(5)
    load(tok, tokb.at[OWN, pl.ds(0, TOK)], 6)
    for p in Z_FIRST:
        load_piece(p)
    load(wdn, wd.at[0], 7)

    barrier = pltpu.get_barrier_semaphore()
    for peer in (x_right, x_left, z_far, y_right, y_left, z_near, twin):
        pl.semaphore_signal(barrier, inc=1, device_id=peer, device_id_type=MESH)

    weights = probs[...] / jnp.sum(probs[...], axis=0, keepdims=True)
    high = weights.astype(BF16)
    middle = (weights - high.astype(F32)).astype(BF16)
    low = (weights - high.astype(F32) - middle.astype(F32)).astype(BF16)
    numbers = ids[...].astype(F32).astype(BF16)
    for k in range(TOP):
        parts = [v[k : k + 1, :] for v in (numbers, high, middle, low)]
        rows = jnp.concatenate([*parts, jnp.zeros((META - 4, TOK), BF16)], axis=0)
        tokb[OWN, TOK:ROWS, k * TOK : (k + 1) * TOK] = rows

    before = lax.broadcasted_iota(jnp.int32, (TOK, TOK), 0)
    after = lax.broadcasted_iota(jnp.int32, (TOK, TOK), 1)
    tri[...] = jnp.where(before < after, 1.0, 0.0).astype(BF16)
    pl.semaphore_wait(barrier, 7)

    slot_number = lax.broadcasted_iota(jnp.int32, (CAP, TOK), 0).astype(F32)

    def dispatch(r, carry):
        routing = tokb[r, pl.ds(TOK, META), :].astype(F32)
        places, shares = [], []
        for e in range(2):
            number = (ex * 2 + e).astype(F32)
            named = jnp.zeros((1, TOK), F32)
            weight = jnp.zeros((1, TOK), F32)
            for k in range(TOP):
                cols = slice(k * TOK, (k + 1) * TOK)
                hit = routing[0:1, cols] == number
                value = routing[1:2, cols] + routing[2:3, cols] + routing[3:4, cols]
                named = named + jnp.where(hit, 1.0, 0.0)
                weight = weight + jnp.where(hit, value, 0.0)
            many = jnp.broadcast_to(named, (16, TOK)).astype(BF16)
            slot = jnp.dot(many, tri[...], preferred_element_type=F32)[0:1, :]
            place = jnp.where(slot_number == slot, jnp.broadcast_to(named, (CAP, TOK)), 0.0)
            places.append(place)
            shares.append(place * weight)
        share = jnp.concatenate(shares, axis=0)
        upper = share.astype(BF16).astype(F32)
        pt[r, :, :] = jnp.concatenate([upper, share - upper], axis=0).T.astype(BF16)
        place = jnp.concatenate(places, axis=0).astype(BF16)
        rows = pl.ds(pl.multiple_of(r * CAP, CAP), CAP)
        for c in range(4):
            cols = slice(c * 512, (c + 1) * 512)
            picked = jnp.dot(place, tokb[r, 0:TOK, cols], preferred_element_type=F32).astype(BF16)
            xs[0, rows, cols] = picked[0:CAP]
            xs[1, rows, cols] = picked[CAP:]
        return carry

    def gate_up(p, *halves):
        e, n = PIECES[p]

        def tile(i, carry):
            rows = pl.ds(pl.multiple_of(i * 640, 640), 640)
            both = jnp.dot(xs[e, rows, :], wg[e, n].reshape(D, 2 * COL), preferred_element_type=F32)
            gate, up = both[:, :COL], both[:, COL:]
            hid[e, rows, n * COL : (n + 1) * COL] = (gate / (1.0 + jnp.exp(-gate)) * up).astype(BF16)
            return carry

        lax.fori_loop(halves[0], halves[-1] + 1, tile, 0)

    def gate_up_part(p, z, rows):
        e, n = PIECES[p]
        width = pl.ds(pl.multiple_of(z * (D // 2), D // 2), D // 2)
        return jnp.dot(
            xs[e, rows, width], wg[e, n, pl.ds(z * 4, 4)].reshape(D // 2, 2 * COL), preferred_element_type=F32
        )

    def gate_up_near(p, half):
        rows = pl.ds(half * 640, 640)
        part[rows, :] = gate_up_part(p, zh, rows)

    def gate_up_far(p):
        e, n = PIECES[p]

        def tile(i, carry):
            rows = pl.ds(pl.multiple_of(i * 640, 640), 640)
            both = part[rows, :] + gate_up_part(p, 1 - zh, rows)
            gate, up = both[:, :COL], both[:, COL:]
            hid[e, rows, n * COL : (n + 1) * COL] = (gate / (1.0 + jnp.exp(-gate)) * up).astype(BF16)
            return carry

        lax.fori_loop(0, 2, tile, 0)

    def own_piece(p):
        e, n = PIECES[p]
        loaded(wg.at[e, n, mine], p)
        start(gu[p].right, gu[p].left)

    def forward(p):
        gu[p].near_in.wait()
        start(gu[p].fwd_r, gu[p].fwd_l)

    def far_start(p):
        gu[p].z_in.wait()
        start(gu[p].zright, gu[p].zleft)

    def far_forward(p):
        gu[p].far_in.wait()
        start(gu[p].zfwd_r, gu[p].zfwd_l)

    own_piece(4)
    loaded(tokb.at[OWN, pl.ds(0, TOK)], 6)
    start(t_z, t_right, t_left, twins[OWN])
    own_piece(5)
    for p in Z_FIRST:
        own_piece(p)
    start(gu[0].z, gu[1].z, gu[4].z)

    forward(4)
    start(gu[4].zl, gu[4].zr, gu[2].z)
    forward(5)
    forward(0)
    near_in.wait()
    start(t_fwd_r, t_fwd_l)
    z_in.wait()
    start(t_zright, t_zleft, twins[ZED], twins[LEFT], twins[RIGHT])
    forward(1)
    forward(2)
    far_start(0)
    forward(3)
    twins_in[0].wait()
    lax.fori_loop(0, 8, dispatch, 0)
    gu[4].across_in.wait()
    start(gu[4].za, gu[3].z, gu[5].z, gu[5].zl, gu[5].zr)
    far_start(1)
    across_in.wait()
    start(twins[ACROSS])
    gu[5].across_in.wait()
    gate_up_near(5, 0)
    far_forward(0)
    far_start(2)
    far_in.wait()
    start(t_zfwd_r, t_zfwd_l, twins[ZLEFT], twins[ZRIGHT])
    far_forward(1)
    gu[4].rest_in.wait()
    gate_up(4, 0)
    gu[0].rest_in.wait()
    gate_up(0, 0)
    far_start(3)
    twins_in[1].wait()
    lax.fori_loop(8, 14, dispatch, 0)
    far_forward(2)
    last_in.wait()
    start(twins[ZACROSS])
    gu[1].rest_in.wait()
    gate_up(1, 0)
    twins_in[2].wait()
    lax.fori_loop(14, SRC, dispatch, 0)
    gate_up(4, 1)
    far_forward(3)
    gate_up(0, 1)
    tokens_sent.wait()
    for peer in (y_right, y_left, z_near, twin):
        pl.semaphore_signal(free_sem, inc=1, device_id=peer, device_id_type=MESH)
    loaded(wd.at[0], 7)
    start(dn[0].z, dn[1].z)
    gate_up(1, 1)
    gu[2].rest_in.wait()
    gate_up(2, 0, 1)
    far_forward(5)
    start(dn[0].right, dn[0].left, dn[1].right, dn[1].left)
    gate_up_near(5, 1)
    gu[3].rest_in.wait()
    gate_up(3, 0, 1)
    gu[5].rest_in.wait()
    gate_up_far(5)
    pl.semaphore_wait(free_sem, 4)

    upper, lower = pl.ds(0, TOK // 2), pl.ds(TOK // 2, TOK // 2)
    every = pl.ds(0, TOK)

    class Return:
        def __init__(self, n, slot, half):
            self.n, self.slot, self.half, self.z_first = n, slot, half, n in RETURN_Z_FIRST
            self.width = width = STEP if self.z_first else 2 * STEP
            pair, self.base = n // 2, n % 2 * 8 * STEP
            self.e, self.row = (0, pair * TOK) if pair < 5 else (1, (pair - 3) * TOK)
            self.twin_row = pair % 2 * TOK
            lane = pl.ds(pair % 4 * 512 + n % 2 * 256, width)

            def mine(col, cols, first=0, rows=TOK):
                return xs.at[self.e, pl.ds(self.row + first, rows), pl.ds(self.base + col, cols)]

            if self.z_first:
                self.z_lands = zbuf.at[RETURN_Z_FIRST.index(n)]
                z = (mine(4 * STEP, 4 * STEP), self.z_lands, z_near)
            else:
                z = (mine(STEP, STEP), tokb.at[14, every, pl.ds(n * STEP, STEP)], z_near)
            rows = TOK // 2
            self.twin_lands = tokb.at[pair, every, pl.ds(self.base, 8 * STEP)]
            theirs = xs.at[1, pl.ds(self.twin_row, TOK), pl.ds(self.base, 8 * STEP)]
            self.moves = dict(
                twin=(theirs, self.twin_lands, twin),
                right1=(mine(2 * width, width, 0, rows), tokb.at[8 + n // 8, upper, lane], y_right),
                left1=(mine(2 * width, width, rows, rows), tokb.at[8 + n // 8, lower, lane], y_left),
                right2=(mine(width, width), tokb.at[10 + n // 8, every, lane], y_right),
                left2=(mine(3 * width, width), tokb.at[12 + n // 8, every, lane], y_left),
                z=z,
            )
            self.ring = sums_sent
            self.twin_in, self.hop_in = Landing(self.twin_lands), Landing(tokb.at[8, every, pl.ds(0, width)])
            self.home_in = Landing(tokb.at[10, every, pl.ds(0, 2 * width)])
            self.z_in = Landing(z[1])
            self.landings = dict(
                twin=self.twin_in, right1=self.hop_in, left1=self.hop_in, right2=self.home_in, left2=self.home_in, z=self.z_in
            )
            column = (((zh + slot // 4) % 2) * 4 + (x + 4 - slot % 4) % 4) * COL + half * STEP
            self.store = pltpu.make_async_copy(
                ob.at[n], out.at[:, pl.ds(pl.multiple_of(column, STEP), STEP)], out_sem
            )

        def start(self, *names):
            for name in names:
                src, dst, device = self.moves[name]
                sent = twins_sent[self.n % 4] if name == "twin" else sums_sent
                start(move(src, dst, device, sent, self.landings[name]))

        def landed(self, name):
            return self.moves[name][1][...].astype(F32)

        def sums(self, col, cols, first=0, rows=TOK):
            return xs[self.e, self.row + first : self.row + first + rows, self.base + col : self.base + col + cols].astype(F32)

        def keep(self, total, col, first=0):
            rows, cols = total.shape
            at = slice(self.row + first, self.row + first + rows)
            xs[self.e, at, self.base + col : self.base + col + cols] = total.astype(BF16)

        def add(self, theirs, cols):
            def some(i, carry):
                at = pl.ds(pl.multiple_of(self.row + i * 64, 64), 64)
                got = theirs[pl.ds(pl.multiple_of(i * 64, 64), 64), :].astype(F32)
                lanes = slice(self.base, self.base + cols)
                xs[self.e, at, lanes] = (xs[self.e, at, lanes].astype(F32) + got).astype(BF16)
                return carry

            lax.fori_loop(0, TOK // 64, some, 0)

        def join_twin(self):
            self.twin_in.wait()
            self.add(self.twin_lands, 8 * STEP)
            self.start(*(("z",) if self.z_first else ("right1", "left1")))

        def second(self):
            width, rows = self.width, TOK // 2
            self.hop_in.wait()
            for there, col, first in (("right", width, 0), ("left", 3 * width, rows)):
                self.keep(self.sums(col, width, first, rows) + self.landed(there + "1"), col, first)
                self.start(there + "2")

        def home(self):
            self.home_in.wait()
            return self.sums(0, self.width) + self.landed("right2") + self.landed("left2")

        def hop(self):
            if self.z_first:
                self.z_in.wait()
                self.add(self.z_lands, 4 * STEP)
                self.start("right1", "left1")
            else:
                self.second()

        def third(self):
            if self.z_first:
                self.second()
            else:
                self.keep(self.home(), 0)
                self.start("z")

        def last(self):
            if self.z_first:
                total = self.home()
            else:
                self.z_in.wait()
                total = self.sums(0, STEP) + self.landed("z")
            ob[self.n] = total.astype(BF16)
            self.store.start()

    sums_sent = Sent(xs.at[:, pl.ds(0, STEPS * TOK // 4), pl.ds(0, 14 * STEP)])
    twins_sent = [Sent(xs.at[1, pl.ds(0, TOK), pl.ds(0, 8 * STEP)]) for _ in range(4)]
    returns, unit_steps = [], []
    for unit in UNITS:
        unit_steps.append([Return(len(returns) + i, slot, half) for i, (slot, half) in enumerate(unit)])
        returns += unit_steps[-1]

    def combine(steps):
        cols = len(steps) * STEP

        def side(mine, carry):
            def where(step):
                row = (1 - mine) * step.twin_row + mine * step.row
                return (1 - mine) + mine * step.e, pl.ds(pl.multiple_of(row, TOK), TOK)

            for (yy, zz), s in RETURN.items():
                r = s + 1 - mine
                total = jnp.dot(pt[r], yb[r, :, 0:cols], preferred_element_type=F32).astype(BF16)
                for i, step in enumerate(steps):
                    place = 4 * zz + yy if step.z_first else 2 * yy + zz
                    e, rows = where(step)
                    at = slice(step.base + place * STEP, step.base + (place + 1) * STEP)
                    xs[e, rows, at] = total[:, i * STEP : (i + 1) * STEP]

            @pl.when(mine == 0)
            def _():
                for step in steps:
                    step.start("twin")

            return carry

        lax.fori_loop(0, 2, side, 0)

    def compute(u):
        steps, unit = unit_steps[u], UNITS[u]
        for step in steps:
            if step.n >= 4:
                twins_sent[step.n % 4].wait()
        for slot, half in unit:
            if slot in (1, 3):
                once("n", half)
            elif slot == 2:
                once("a", half)
            elif slot == 4:
                once("f", half)
            elif slot in (5, 7):
                once("w", half)
            elif slot == 6:
                once("A", half)
        for e in range(2):
            shard = jnp.concatenate([wd[slot, e, :, half * STEP : (half + 1) * STEP] for slot, half in unit], axis=1)
            y_e = jnp.dot(hid[e], shard, preferred_element_type=F32).astype(BF16)
            for part_at in (0, 2 * CAP):
                rows = slice(part_at + e * CAP, part_at + (e + 1) * CAP)
                yb[:, rows, 0 : len(unit) * STEP] = y_e.reshape(SRC, CAP, -1)
        combine(steps)

    made = set()

    def once(what, half):
        if (what, half) in made:
            return
        made.add((what, half))
        d = dn[half]
        if what == "n":
            d.near_in.wait()
            start(d.fwd_r, d.fwd_l)
        elif what == "a":
            once("n", half)
            d.across_in.wait()
        elif what == "f":
            d.z_in.wait()
            start(d.zright, d.zleft)
        elif what == "w":
            once("f", half)
            d.far_in.wait()
        elif what == "F":
            once("w", half)
            start(d.zfwd_r, d.zfwd_l)
        elif what == "g":
            once("a", half)
            start(d.za)
        elif what == "A":
            once("g" if half in Z_LAST else "F", half)
            d.last_in.wait()

    do = {
        "C": compute, "T": lambda n: returns[n].join_twin(), "S": lambda n: returns[n].hop(),
        "H": lambda n: returns[n].third(), "L": lambda n: returns[n].last(),
        **{what: functools.partial(once, what) for what in "nfFg"},
    }
    for what, n in PLAN:
        do[what](n)
    sums_sent.wait()
    for n in range(STEPS - 4, STEPS):
        twins_sent[n % 4].wait()
    pltpu.make_async_copy(ob, ob, out_sem).wait()
    for group in (*gu, *dn):
        group.sent.wait()


def shards(tokens, expert_ids, route_probs, w_gate_up, w_down):
    any_spec = pl.BlockSpec(memory_space=pl.ANY)
    vmem_spec = pl.BlockSpec(memory_space=pltpu.VMEM)
    return pl.pallas_call(
        kernel,
        out_shape=jax.ShapeDtypeStruct((TOK, D), BF16),
        in_specs=[any_spec, vmem_spec, vmem_spec, any_spec, any_spec],
        out_specs=any_spec,
        scratch_shapes=[
            pltpu.VMEM((SRC, ROWS, D), BF16),
            pltpu.VMEM((2, 3, SHARDS, COL, 2 * COL), BF16),
            pltpu.VMEM((SHARDS, 2, FF, COL), BF16),
            pltpu.VMEM((2, SRC * CAP, D), BF16),
            pltpu.VMEM((2, SRC * CAP, FF), BF16),
            pltpu.VMEM((SRC, TOK, 4 * CAP), BF16),
            pltpu.VMEM((SRC, 4 * CAP, COL), BF16),
            pltpu.VMEM((TOK, TOK), BF16),
            pltpu.VMEM((len(RETURN_Z_FIRST), TOK, 4 * STEP), BF16),
            pltpu.VMEM((STEPS, TOK, STEP), BF16),
            pltpu.VMEM((SRC * CAP, 2 * COL), F32),
            pltpu.SemaphoreType.DMA((8,)),
            pltpu.SemaphoreType.DMA((SENDS,)),
            pltpu.SemaphoreType.DMA((LANDINGS,)),
            pltpu.SemaphoreType.DMA,
            pltpu.SemaphoreType.REGULAR,
        ],
        compiler_params=pltpu.CompilerParams(
            collective_id=0, has_side_effects=True, vmem_limit_bytes=67_000_000
        ),
    )(tokens, expert_ids.T, route_probs.T, w_gate_up, w_down)


def solution(mesh):
    spec = P(("dp", "expert"), None)
    in_specs = (spec, spec, spec, P("expert", "dp", None), P("expert", None, "dp"))
    return jax.shard_map(shards, mesh=mesh, in_specs=in_specs, out_specs=spec, check_vma=False)
```

```python
import functools

import jax
import jax.numpy as jnp
from jax import lax
from jax.experimental import pallas as pl
from jax.experimental.pallas import tpu as pltpu
from jax.sharding import PartitionSpec as P

MESH = pl.DeviceIdType.MESH
F32 = jnp.float32
BF16 = jnp.bfloat16

TOK = 256
META = 16
META_COLS = 512
ROWS = TOK + META
HALF = TOK // 2
D = 2048
FF = 768
TOP = 8
CAP = 80
SRC = 16
COL = 256
SHARDS = 8
STEPS = 16
STEP = COL // 2
LANDINGS = 2 * 8 + 4 * 4 + 3 + 4 + 2 * 5 + 16 * 4
SENDS = 2 + 6 + 2 + 1 + 4

OWN, ZED, LEFT, RIGHT, ACROSS, ZLEFT, ZRIGHT, ZACROSS = range(0, 16, 2)
RETURN = {
    (0, 0): OWN, (0, 1): ZED, (1, 0): RIGHT, (1, 1): ZRIGHT,
    (2, 0): ACROSS, (2, 1): ZACROSS, (3, 0): LEFT, (3, 1): ZLEFT,
}
PIECES = [(e, n) for e in range(2) for n in range(3)]
Z_FIRST = (0, 1, 2, 3)
X_FIRST = (4, 5)
Z_ACROSS = 4

UNITS = (
    ((0, 0), (0, 1)), ((1, 0), (3, 0)), ((1, 1), (3, 1)), ((4, 0), (4, 1)), ((2, 0), (2, 1)), ((5, 0), (7, 0)), ((5, 1), (7, 1)), ((6, 0),), ((6, 1),),
)
RETURN_Z_FIRST = (4, 6, 10, 12, 14)
Z_LAST = ()
PLAN = (
    ("C", 0), ("T", 0), ("T", 1), ("S", 0), ("n", 0), ("S", 1), ("C", 1), ("T", 2), ("T", 3), ("H", 1),
    ("n", 1), ("f", 0), ("f", 1), ("S", 2), ("H", 0), ("C", 2), ("C", 3), ("T", 4), ("T", 5), ("S", 3),
    ("T", 6), ("C", 4), ("S", 5), ("T", 9), ("S", 4), ("H", 3), ("T", 8), ("T", 7), ("S", 9), ("C", 5),
    ("S", 8), ("S", 6), ("H", 5), ("F", 0), ("L", 3), ("H", 4), ("T", 10), ("T", 11), ("H", 9), ("S", 7),
    ("F", 1), ("C", 6), ("T", 12), ("S", 11), ("C", 7), ("T", 13), ("S", 10), ("H", 6), ("T", 14), ("C", 8),
    ("T", 15), ("S", 13), ("S", 12), ("H", 11), ("L", 4), ("L", 9), ("S", 15), ("L", 6), ("H", 8), ("S", 14),
    ("H", 13), ("H", 12), ("H", 7), ("H", 10), ("L", 1), ("H", 2), ("L", 11), ("L", 5), ("L", 0), ("H", 15),
    ("H", 14), ("L", 10), ("L", 2), ("L", 12), ("L", 7), ("L", 13), ("L", 8), ("L", 15), ("L", 14),
)


def kernel(
    tok, ids, probs, wgu, wdn, out,
    tokb, wg, wd, xs, hid, pt, yb, tri, zbuf, ob, part,
    local_sem, send_sem, recv_sem, out_sem, free_sem,
):
    dp, ex = lax.axis_index("dp"), lax.axis_index("expert")
    zh, x = dp // 4, dp % 4
    y, zl, core = ex // 4, (ex // 2) % 2, ex % 2
    xl, xr, xa = (x + 3) % 4, (x + 1) % 4, (x + 2) % 4

    def at_dp(zhi, xx):
        return (zhi * 4 + xx, ex)

    def at_ex(yy, zz, cc):
        return (dp, (yy * 2 + zz) * 2 + cc)

    x_right, x_left, z_far = at_dp(zh, xr), at_dp(zh, xl), at_dp(1 - zh, x)
    y_right, y_left = at_ex((y + 1) % 4, zl, core), at_ex((y + 3) % 4, zl, core)
    z_near, twin = at_ex(y, 1 - zl, core), at_ex(y, zl, 1 - core)

    counts = dict(send=0, recv=0)

    def semaphore(kind):
        counts[kind] += 1
        return (send_sem if kind == "send" else recv_sem).at[counts[kind] - 1]

    def described(src, dst, send, recv, device):
        return pltpu.make_async_remote_copy(
            src_ref=src, dst_ref=dst, send_sem=send, recv_sem=recv, device_id=device, device_id_type=MESH
        )

    class Landing:
        def __init__(self, ref):
            self.ref, self.semaphore = ref, semaphore("recv")

        def wait(self):
            described(self.ref, self.ref, all_sent[0], self.semaphore, twin).wait_recv()

    class Sent:
        def __init__(self, ref):
            self.ref, self.semaphore = ref, semaphore("send")
            all_sent.append(self.semaphore)

        def wait(self):
            described(self.ref, self.ref, self.semaphore, recv_sem.at[0], twin).wait_send()

    all_sent = []

    def move(src, dst, device, sent, landing):
        return functools.partial(described, src, dst, sent.semaphore, landing.semaphore, device)

    def start(*moves):
        for m in moves:
            for each in m if isinstance(m, tuple) else (m,):
                each().start()

    first, second = pl.ds(0, HALF), pl.ds(HALF, HALF)
    body, routing_rows = (pl.ds(0, TOK),), (pl.ds(TOK, META), pl.ds(0, META_COLS))

    def blocks(n):
        return tokb.at[(pl.ds(0, n), *body)], tokb.at[(pl.ds(0, n), *routing_rows)]

    class Both:
        def __init__(self, kind, n):
            self.tokens, self.routing = (kind(ref) for ref in blocks(n))

        def wait(self):
            self.tokens.wait()
            self.routing.wait()

    tokens_sent = Both(Sent, 15)
    z_in, near_in, across_in, far_in, last_in = (Both(Landing, n) for n in (1, 2, 1, 2, 1))
    twins_in = [Both(Landing, n) for n in (4, 3, 1)]

    def block(src, dst, device, landing, rows=None):
        routing = move(
            tokb.at[(src, *routing_rows)], tokb.at[(dst, *routing_rows)], device, tokens_sent.routing, landing.routing
        )
        if rows is None:
            rows = pl.ds(0, TOK)
        tokens = move(tokb.at[src, rows], tokb.at[dst, rows], device, tokens_sent.tokens, landing.tokens)
        return (tokens,) if rows is second else (routing, tokens)

    t_z = block(OWN, ZED, z_near, z_in)
    t_right, t_left = block(OWN, LEFT, y_right, near_in), block(OWN, RIGHT, y_left, near_in)
    t_fwd_r = block(LEFT, ACROSS, y_right, across_in, first)
    t_fwd_l = block(RIGHT, ACROSS, y_left, across_in, second)
    t_zright, t_zleft = block(ZED, ZLEFT, y_right, far_in), block(ZED, ZRIGHT, y_left, far_in)
    t_zfwd_r = block(ZLEFT, ZACROSS, y_right, last_in, first)
    t_zfwd_l = block(ZRIGHT, ZACROSS, y_left, last_in, second)
    waves = {OWN: 0, ZED: 0, LEFT: 0, RIGHT: 0, ACROSS: 1, ZLEFT: 1, ZRIGHT: 1, ZACROSS: 2}
    twins = {s: block(s, s + 1, twin, twins_in[w]) for s, w in waves.items()}

    class GateUp:
        def __init__(self, p):
            e, n = PIECES[p]
            top, low = pl.ds(0, COL // 2), pl.ds(COL // 2, COL // 2)
            far = 1 - zh

            def shards(k):
                return wg.at[e, n, pl.ds(0, k)]

            self.sent, self.near_in = Sent(shards(7)), Landing(shards(2))
            if p in Z_FIRST:
                self.z_in, self.far_in = Landing(shards(1)), Landing(shards(2))
                self.rest_in = across_in = Landing(shards(2))
                z_in, last_in = self.z_in, self.rest_in
            elif p == Z_ACROSS:
                self.across_in, self.rest_in = Landing(shards(1)), Landing(shards(4))
                across_in = self.across_in
                z_in = self.far_in = last_in = self.rest_in
            else:
                self.across_in, self.far_in = Landing(shards(1)), Landing(shards(2))
                self.rest_in, across_in = Landing(shards(2)), self.across_in
                z_in = last_in = self.rest_in

            def same(device, z, xx, landing, rows=slice(None)):
                ref = wg.at[e, n, z * 4 + xx, rows]
                return move(ref, ref, device, self.sent, landing)

            self.right, self.left = same(x_right, zh, x, self.near_in), same(x_left, zh, x, self.near_in)
            self.fwd_r, self.fwd_l = same(x_right, zh, xl, across_in, top), same(x_left, zh, xr, across_in, low)
            self.z = same(z_far, zh, x, z_in)
            if p in X_FIRST:
                self.zl, self.zr = same(z_far, zh, xl, self.far_in), same(z_far, zh, xr, self.far_in)
            else:
                self.zright, self.zleft = same(x_right, far, x, self.far_in), same(x_left, far, x, self.far_in)
            if p == Z_ACROSS:
                self.za = same(z_far, zh, xa, last_in)
            else:
                self.zfwd_r, self.zfwd_l = same(x_right, far, xl, last_in, top), same(x_left, far, xr, last_in, low)

    class Down:
        def __init__(self, half):
            top, low = pl.ds(0, FF // 2), pl.ds(FF // 2, FF // 2)
            cols = pl.ds(half * STEP, STEP)

            def slots(k):
                return wd.at[pl.ds(0, k), :, :, cols]

            self.sent = Sent(slots(7))
            self.near_in, self.across_in, self.z_in, self.far_in, self.last_in = (
                Landing(slots(k)) for k in (2, 1, 1, 2, 1)
            )

            def to(device, src, dst, landing, rows=slice(None)):
                return move(wd.at[src, :, rows, cols], wd.at[dst, :, rows, cols], device, self.sent, landing)

            self.right, self.left = to(x_right, 0, 1, self.near_in), to(x_left, 0, 3, self.near_in)
            self.z = to(z_far, 0, 4, self.z_in)
            self.fwd_r, self.fwd_l = to(x_right, 1, 2, self.across_in, top), to(x_left, 3, 2, self.across_in, low)
            self.zright, self.zleft = to(x_right, 4, 5, self.far_in), to(x_left, 4, 7, self.far_in)
            if half in Z_LAST:
                self.za = to(z_far, 2, 6, self.last_in)
            else:
                self.zfwd_r, self.zfwd_l = to(x_right, 5, 6, self.last_in, top), to(x_left, 7, 6, self.last_in, low)

    gu = [GateUp(p) for p in range(6)]
    dn = [Down(0), Down(1)]

    mine = zh * 4 + x
    def load(src, dst, name):
        pltpu.make_async_copy(src, dst, local_sem.at[name]).start()

    def loaded(dst, name):
        pltpu.make_async_copy(dst, dst, local_sem.at[name]).wait()

    def load_piece(p):
        e, n = PIECES[p]
        load(wgu.at[e, :, pl.ds(n * COL, COL)], wg.at[e, n, mine, :, pl.ds(0, COL)], p)
        load(wgu.at[e, :, pl.ds(FF + n * COL, COL)], wg.at[e, n, mine, :, pl.ds(COL, COL)], p)

    load_piece(4)
    load_piece(5)
    load(tok, tokb.at[OWN, pl.ds(0, TOK)], 6)
    for p in Z_FIRST:
        load_piece(p)
    load(wdn, wd.at[0], 7)

    barrier = pltpu.get_barrier_semaphore()
    for peer in (x_right, x_left, z_far, y_right, y_left, z_near, twin):
        pl.semaphore_signal(barrier, inc=1, device_id=peer, device_id_type=MESH)

    weights = probs[...] / jnp.sum(probs[...], axis=0, keepdims=True)
    high = weights.astype(BF16)
    middle = (weights - high.astype(F32)).astype(BF16)
    low = (weights - high.astype(F32) - middle.astype(F32)).astype(BF16)
    numbers = ids[...].astype(F32).astype(BF16)
    for lane in range(2):
        rows = [v[k : k + 1, :] for v in (numbers, high, middle, low) for k in range(lane, TOP, 2)]
        tokb[OWN, TOK:ROWS, lane * TOK : (lane + 1) * TOK] = jnp.concatenate(rows, axis=0)

    before = lax.broadcasted_iota(jnp.int32, (TOK, TOK), 0)
    after = lax.broadcasted_iota(jnp.int32, (TOK, TOK), 1)
    tri[...] = jnp.where(before < after, 1.0, 0.0).astype(BF16)
    pl.semaphore_wait(barrier, 7)

    slot_number = lax.broadcasted_iota(jnp.int32, (CAP, TOK), 0).astype(F32)

    def dispatch(r, carry):
        routing = tokb[r, pl.ds(TOK, META), pl.ds(0, META_COLS)].astype(F32)
        places, shares = [], []
        for e in range(2):
            number = (ex * 2 + e).astype(F32)
            named = jnp.zeros((1, TOK), F32)
            weight = jnp.zeros((1, TOK), F32)
            for k in range(TOP):
                cols = slice(k % 2 * TOK, (k % 2 + 1) * TOK)
                mark, high, middle, low = (routing[4 * i + k // 2 : 4 * i + k // 2 + 1, cols] for i in range(4))
                hit = mark == number
                value = high + middle + low
                named = named + jnp.where(hit, 1.0, 0.0)
                weight = weight + jnp.where(hit, value, 0.0)
            many = jnp.broadcast_to(named, (16, TOK)).astype(BF16)
            slot = jnp.dot(many, tri[...], preferred_element_type=F32)[0:1, :]
            place = jnp.where(slot_number == slot, jnp.broadcast_to(named, (CAP, TOK)), 0.0)
            places.append(place)
            shares.append(place * weight)
        share = jnp.concatenate(shares, axis=0)
        upper = share.astype(BF16).astype(F32)
        pt[r, :, :] = jnp.concatenate([upper, share - upper], axis=0).T.astype(BF16)
        place = jnp.concatenate(places, axis=0).astype(BF16)
        rows = pl.ds(pl.multiple_of(r * CAP, CAP), CAP)
        for c in range(4):
            cols = slice(c * 512, (c + 1) * 512)
            picked = jnp.dot(place, tokb[r, 0:TOK, cols], preferred_element_type=F32).astype(BF16)
            xs[0, rows, cols] = picked[0:CAP]
            xs[1, rows, cols] = picked[CAP:]
        return carry

    def gate_up(p, *halves):
        e, n = PIECES[p]

        def tile(i, carry):
            rows = pl.ds(pl.multiple_of(i * 640, 640), 640)
            both = jnp.dot(xs[e, rows, :], wg[e, n].reshape(D, 2 * COL), preferred_element_type=F32)
            gate, up = both[:, :COL], both[:, COL:]
            hid[e, rows, n * COL : (n + 1) * COL] = (gate / (1.0 + jnp.exp(-gate)) * up).astype(BF16)
            return carry

        lax.fori_loop(halves[0], halves[-1] + 1, tile, 0)

    def gate_up_part(p, z, rows):
        e, n = PIECES[p]
        width = pl.ds(pl.multiple_of(z * (D // 2), D // 2), D // 2)
        return jnp.dot(
            xs[e, rows, width], wg[e, n, pl.ds(z * 4, 4)].reshape(D // 2, 2 * COL), preferred_element_type=F32
        )

    def gate_up_near(p, half):
        rows = pl.ds(half * 640, 640)
        part[rows, :] = gate_up_part(p, zh, rows)

    def gate_up_far(p):
        e, n = PIECES[p]

        def tile(i, carry):
            rows = pl.ds(pl.multiple_of(i * 640, 640), 640)
            both = part[rows, :] + gate_up_part(p, 1 - zh, rows)
            gate, up = both[:, :COL], both[:, COL:]
            hid[e, rows, n * COL : (n + 1) * COL] = (gate / (1.0 + jnp.exp(-gate)) * up).astype(BF16)
            return carry

        lax.fori_loop(0, 2, tile, 0)

    def own_piece(p):
        e, n = PIECES[p]
        loaded(wg.at[e, n, mine], p)
        start(gu[p].right, gu[p].left)

    def forward(p):
        gu[p].near_in.wait()
        start(gu[p].fwd_r, gu[p].fwd_l)

    def far_start(p):
        gu[p].z_in.wait()
        start(gu[p].zright, gu[p].zleft)

    def far_forward(p):
        gu[p].far_in.wait()
        start(gu[p].zfwd_r, gu[p].zfwd_l)

    own_piece(4)
    loaded(tokb.at[OWN, pl.ds(0, TOK)], 6)
    start(t_z, t_right, t_left, twins[OWN])
    own_piece(5)
    for p in Z_FIRST:
        own_piece(p)
    start(gu[0].z, gu[1].z, gu[4].z)

    forward(4)
    start(gu[4].zl, gu[4].zr, gu[2].z)
    forward(5)
    forward(0)
    near_in.wait()
    start(t_fwd_r, t_fwd_l)
    z_in.wait()
    start(t_zright, t_zleft, twins[ZED], twins[LEFT], twins[RIGHT])
    forward(1)
    forward(2)
    far_start(0)
    forward(3)
    twins_in[0].wait()
    lax.fori_loop(0, 8, dispatch, 0)
    gu[4].across_in.wait()
    start(gu[4].za, gu[3].z, gu[5].z, gu[5].zl, gu[5].zr)
    far_start(1)
    across_in.wait()
    start(twins[ACROSS])
    gu[5].across_in.wait()
    gate_up_near(5, 0)
    far_forward(0)
    far_start(2)
    far_in.wait()
    start(t_zfwd_r, t_zfwd_l, twins[ZLEFT], twins[ZRIGHT])
    far_forward(1)
    gu[4].rest_in.wait()
    gate_up(4, 0)
    gu[0].rest_in.wait()
    gate_up(0, 0)
    far_start(3)
    twins_in[1].wait()
    lax.fori_loop(8, 14, dispatch, 0)
    far_forward(2)
    last_in.wait()
    start(twins[ZACROSS])
    gu[1].rest_in.wait()
    gate_up(1, 0)
    twins_in[2].wait()
    lax.fori_loop(14, SRC, dispatch, 0)
    gate_up(4, 1)
    far_forward(3)
    gate_up(0, 1)
    tokens_sent.wait()
    for peer in (y_right, y_left, z_near, twin):
        pl.semaphore_signal(free_sem, inc=1, device_id=peer, device_id_type=MESH)
    loaded(wd.at[0], 7)
    start(dn[0].z, dn[1].z)
    gate_up(1, 1)
    gu[2].rest_in.wait()
    gate_up(2, 0, 1)
    far_forward(5)
    start(dn[0].right, dn[0].left, dn[1].right, dn[1].left)
    gate_up_near(5, 1)
    gu[3].rest_in.wait()
    gate_up(3, 0, 1)
    gu[5].rest_in.wait()
    gate_up_far(5)
    pl.semaphore_wait(free_sem, 4)

    upper, lower = pl.ds(0, TOK // 2), pl.ds(TOK // 2, TOK // 2)
    every = pl.ds(0, TOK)

    class Return:
        def __init__(self, n, slot, half):
            self.n, self.slot, self.half, self.z_first = n, slot, half, n in RETURN_Z_FIRST
            self.width = width = STEP if self.z_first else 2 * STEP
            pair, self.base = n // 2, n % 2 * 8 * STEP
            self.e, self.row = (0, pair * TOK) if pair < 5 else (1, (pair - 3) * TOK)
            self.twin_row = pair % 2 * TOK
            lane = pl.ds(pair % 4 * 512 + n % 2 * 256, width)

            def mine(col, cols, first=0, rows=TOK):
                return xs.at[self.e, pl.ds(self.row + first, rows), pl.ds(self.base + col, cols)]

            if self.z_first:
                self.z_lands = zbuf.at[RETURN_Z_FIRST.index(n)]
                z = (mine(4 * STEP, 4 * STEP), self.z_lands, z_near)
            else:
                z = (mine(STEP, STEP), tokb.at[14, every, pl.ds(n * STEP, STEP)], z_near)
            rows = TOK // 2
            self.twin_lands = tokb.at[pair, every, pl.ds(self.base, 8 * STEP)]
            theirs = xs.at[1, pl.ds(self.twin_row, TOK), pl.ds(self.base, 8 * STEP)]
            self.moves = dict(
                twin=(theirs, self.twin_lands, twin),
                right1=(mine(2 * width, width, 0, rows), tokb.at[8 + n // 8, upper, lane], y_right),
                left1=(mine(2 * width, width, rows, rows), tokb.at[8 + n // 8, lower, lane], y_left),
                right2=(mine(width, width), tokb.at[10 + n // 8, every, lane], y_right),
                left2=(mine(3 * width, width), tokb.at[12 + n // 8, every, lane], y_left),
                z=z,
            )
            self.ring = sums_sent
            self.twin_in, self.hop_in = Landing(self.twin_lands), Landing(tokb.at[8, every, pl.ds(0, width)])
            self.home_in = Landing(tokb.at[10, every, pl.ds(0, 2 * width)])
            self.z_in = Landing(z[1])
            self.landings = dict(
                twin=self.twin_in, right1=self.hop_in, left1=self.hop_in, right2=self.home_in, left2=self.home_in, z=self.z_in
            )
            column = (((zh + slot // 4) % 2) * 4 + (x + 4 - slot % 4) % 4) * COL + half * STEP
            self.store = pltpu.make_async_copy(
                ob.at[n], out.at[:, pl.ds(pl.multiple_of(column, STEP), STEP)], out_sem
            )

        def start(self, *names):
            for name in names:
                src, dst, device = self.moves[name]
                sent = twins_sent[self.n % 4] if name == "twin" else sums_sent
                start(move(src, dst, device, sent, self.landings[name]))

        def landed(self, name):
            return self.moves[name][1][...].astype(F32)

        def sums(self, col, cols, first=0, rows=TOK):
            return xs[self.e, self.row + first : self.row + first + rows, self.base + col : self.base + col + cols].astype(F32)

        def keep(self, total, col, first=0):
            rows, cols = total.shape
            at = slice(self.row + first, self.row + first + rows)
            xs[self.e, at, self.base + col : self.base + col + cols] = total.astype(BF16)

        def add(self, theirs, cols):
            def some(i, carry):
                at = pl.ds(pl.multiple_of(self.row + i * 64, 64), 64)
                got = theirs[pl.ds(pl.multiple_of(i * 64, 64), 64), :].astype(F32)
                lanes = slice(self.base, self.base + cols)
                xs[self.e, at, lanes] = (xs[self.e, at, lanes].astype(F32) + got).astype(BF16)
                return carry

            lax.fori_loop(0, TOK // 64, some, 0)

        def join_twin(self):
            self.twin_in.wait()
            self.add(self.twin_lands, 8 * STEP)
            self.start(*(("z",) if self.z_first else ("right1", "left1")))

        def second(self):
            width, rows = self.width, TOK // 2
            self.hop_in.wait()
            for there, col, first in (("right", width, 0), ("left", 3 * width, rows)):
                self.keep(self.sums(col, width, first, rows) + self.landed(there + "1"), col, first)
                self.start(there + "2")

        def home(self):
            self.home_in.wait()
            return self.sums(0, self.width) + self.landed("right2") + self.landed("left2")

        def hop(self):
            if self.z_first:
                self.z_in.wait()
                self.add(self.z_lands, 4 * STEP)
                self.start("right1", "left1")
            else:
                self.second()

        def third(self):
            if self.z_first:
                self.second()
            else:
                self.keep(self.home(), 0)
                self.start("z")

        def last(self):
            if self.z_first:
                total = self.home()
            else:
                self.z_in.wait()
                total = self.sums(0, STEP) + self.landed("z")
            ob[self.n] = total.astype(BF16)
            self.store.start()

    sums_sent = Sent(xs.at[:, pl.ds(0, STEPS * TOK // 4), pl.ds(0, 14 * STEP)])
    twins_sent = [Sent(xs.at[1, pl.ds(0, TOK), pl.ds(0, 8 * STEP)]) for _ in range(4)]
    returns, unit_steps = [], []
    for unit in UNITS:
        unit_steps.append([Return(len(returns) + i, slot, half) for i, (slot, half) in enumerate(unit)])
        returns += unit_steps[-1]

    def combine(steps):
        cols = len(steps) * STEP

        def side(mine, carry):
            def where(step):
                row = (1 - mine) * step.twin_row + mine * step.row
                return (1 - mine) + mine * step.e, pl.ds(pl.multiple_of(row, TOK), TOK)

            for (yy, zz), s in RETURN.items():
                r = s + 1 - mine
                total = jnp.dot(pt[r], yb[r, :, 0:cols], preferred_element_type=F32).astype(BF16)
                for i, step in enumerate(steps):
                    place = 4 * zz + yy if step.z_first else 2 * yy + zz
                    e, rows = where(step)
                    at = slice(step.base + place * STEP, step.base + (place + 1) * STEP)
                    xs[e, rows, at] = total[:, i * STEP : (i + 1) * STEP]

            @pl.when(mine == 0)
            def _():
                for step in steps:
                    step.start("twin")

            return carry

        lax.fori_loop(0, 2, side, 0)

    def compute(u):
        steps, unit = unit_steps[u], UNITS[u]
        for step in steps:
            if step.n >= 4:
                twins_sent[step.n % 4].wait()
        for slot, half in unit:
            if slot in (1, 3):
                once("n", half)
            elif slot == 2:
                once("a", half)
            elif slot == 4:
                once("f", half)
            elif slot in (5, 7):
                once("w", half)
            elif slot == 6:
                once("A", half)
        for e in range(2):
            shard = jnp.concatenate([wd[slot, e, :, half * STEP : (half + 1) * STEP] for slot, half in unit], axis=1)
            y_e = jnp.dot(hid[e], shard, preferred_element_type=F32).astype(BF16)
            for part_at in (0, 2 * CAP):
                rows = slice(part_at + e * CAP, part_at + (e + 1) * CAP)
                yb[:, rows, 0 : len(unit) * STEP] = y_e.reshape(SRC, CAP, -1)
        combine(steps)

    made = set()

    def once(what, half):
        if (what, half) in made:
            return
        made.add((what, half))
        d = dn[half]
        if what == "n":
            d.near_in.wait()
            start(d.fwd_r, d.fwd_l)
        elif what == "a":
            once("n", half)
            d.across_in.wait()
        elif what == "f":
            d.z_in.wait()
            start(d.zright, d.zleft)
        elif what == "w":
            once("f", half)
            d.far_in.wait()
        elif what == "F":
            once("w", half)
            start(d.zfwd_r, d.zfwd_l)
        elif what == "g":
            once("a", half)
            start(d.za)
        elif what == "A":
            once("g" if half in Z_LAST else "F", half)
            d.last_in.wait()

    do = {
        "C": compute, "T": lambda n: returns[n].join_twin(), "S": lambda n: returns[n].hop(),
        "H": lambda n: returns[n].third(), "L": lambda n: returns[n].last(),
        **{what: functools.partial(once, what) for what in "nfFg"},
    }
    for what, n in PLAN:
        do[what](n)
    sums_sent.wait()
    for n in range(STEPS - 4, STEPS):
        twins_sent[n % 4].wait()
    pltpu.make_async_copy(ob, ob, out_sem).wait()
    for group in (*gu, *dn):
        group.sent.wait()


def shards(tokens, expert_ids, route_probs, w_gate_up, w_down):
    any_spec = pl.BlockSpec(memory_space=pl.ANY)
    vmem_spec = pl.BlockSpec(memory_space=pltpu.VMEM)
    return pl.pallas_call(
        kernel,
        out_shape=jax.ShapeDtypeStruct((TOK, D), BF16),
        in_specs=[any_spec, vmem_spec, vmem_spec, any_spec, any_spec],
        out_specs=any_spec,
        scratch_shapes=[
            pltpu.VMEM((SRC, ROWS, D), BF16),
            pltpu.VMEM((2, 3, SHARDS, COL, 2 * COL), BF16),
            pltpu.VMEM((SHARDS, 2, FF, COL), BF16),
            pltpu.VMEM((2, SRC * CAP, D), BF16),
            pltpu.VMEM((2, SRC * CAP, FF), BF16),
            pltpu.VMEM((SRC, TOK, 4 * CAP), BF16),
            pltpu.VMEM((SRC, 4 * CAP, COL), BF16),
            pltpu.VMEM((TOK, TOK), BF16),
            pltpu.VMEM((len(RETURN_Z_FIRST), TOK, 4 * STEP), BF16),
            pltpu.VMEM((STEPS, TOK, STEP), BF16),
            pltpu.VMEM((SRC * CAP, 2 * COL), F32),
            pltpu.SemaphoreType.DMA((8,)),
            pltpu.SemaphoreType.DMA((SENDS,)),
            pltpu.SemaphoreType.DMA((LANDINGS,)),
            pltpu.SemaphoreType.DMA,
            pltpu.SemaphoreType.REGULAR,
        ],
        compiler_params=pltpu.CompilerParams(
            collective_id=0, has_side_effects=True, vmem_limit_bytes=67_000_000
        ),
    )(tokens, expert_ids.T, route_probs.T, w_gate_up, w_down)


def solution(mesh):
    spec = P(("dp", "expert"), None)
    in_specs = (spec, spec, spec, P("expert", "dp", None), P("expert", None, "dp"))
    return jax.shard_map(shards, mesh=mesh, in_specs=in_specs, out_specs=spec, check_vma=False)
```

```python
import functools

import jax
import jax.numpy as jnp
from jax import lax
from jax.experimental import pallas as pl
from jax.experimental.pallas import tpu as pltpu
from jax.sharding import PartitionSpec as P

MESH = pl.DeviceIdType.MESH
F32 = jnp.float32
BF16 = jnp.bfloat16

TOK = 256
META = 16
META_COLS = 512
ROWS = TOK + META
HALF = TOK // 2
D = 2048
FF = 768
TOP = 8
CAP = 80
SRC = 16
COL = 256
SHARDS = 8
STEPS = 16
STEP = COL // 2
LANDINGS = 2 * 8 + 4 * 4 + 3 + 3 + 2 * 5 + 16 * 4
SENDS = 2 + 6 + 2 + 1 + 4

OWN, ZED, LEFT, RIGHT, ACROSS, ZLEFT, ZRIGHT, ZACROSS = range(0, 16, 2)
RETURN = {
    (0, 0): OWN, (0, 1): ZED, (1, 0): RIGHT, (1, 1): ZRIGHT,
    (2, 0): ACROSS, (2, 1): ZACROSS, (3, 0): LEFT, (3, 1): ZLEFT,
}
PIECES = [(e, n) for e in range(2) for n in range(3)]
Z_FIRST = (0, 1, 2, 3)
X_FIRST = (4, 5)
Z_ACROSS = 4

UNITS = (
    ((0, 0), (0, 1)), ((1, 0), (3, 0)), ((1, 1), (3, 1)), ((4, 0), (4, 1)), ((2, 0), (2, 1)), ((5, 0), (7, 0)), ((5, 1), (7, 1)), ((6, 0),), ((6, 1),),
)
RETURN_Z_FIRST = (4, 6, 10, 12, 14)
Z_LAST = ()
PLAN = (
    ("C", 0), ("T", 0), ("T", 1), ("S", 0), ("n", 0), ("S", 1), ("C", 1), ("T", 2), ("T", 3), ("H", 1),
    ("n", 1), ("f", 0), ("f", 1), ("S", 2), ("H", 0), ("C", 2), ("C", 3), ("T", 4), ("T", 5), ("S", 3),
    ("T", 6), ("C", 4), ("S", 5), ("T", 9), ("S", 4), ("H", 3), ("T", 8), ("T", 7), ("S", 9), ("C", 5),
    ("S", 8), ("S", 6), ("H", 5), ("F", 0), ("L", 3), ("H", 4), ("T", 10), ("T", 11), ("H", 9), ("S", 7),
    ("F", 1), ("C", 6), ("T", 12), ("S", 11), ("C", 7), ("T", 13), ("S", 10), ("H", 6), ("T", 14), ("C", 8),
    ("T", 15), ("S", 13), ("S", 12), ("H", 11), ("L", 4), ("L", 9), ("S", 15), ("L", 6), ("H", 8), ("S", 14),
    ("H", 13), ("H", 12), ("H", 7), ("H", 10), ("L", 1), ("H", 2), ("L", 11), ("L", 5), ("L", 0), ("H", 15),
    ("H", 14), ("L", 10), ("L", 2), ("L", 12), ("L", 7), ("L", 13), ("L", 8), ("L", 15), ("L", 14),
)


def kernel(
    tok, ids, probs, wgu, wdn, out,
    tokb, wg, wd, xs, hid, pt, yb, tri, zbuf, ob, part,
    local_sem, send_sem, recv_sem, out_sem, free_sem,
):
    dp, ex = lax.axis_index("dp"), lax.axis_index("expert")
    zh, x = dp // 4, dp % 4
    y, zl, core = ex // 4, (ex // 2) % 2, ex % 2
    xl, xr, xa = (x + 3) % 4, (x + 1) % 4, (x + 2) % 4

    def at_dp(zhi, xx):
        return (zhi * 4 + xx, ex)

    def at_ex(yy, zz, cc):
        return (dp, (yy * 2 + zz) * 2 + cc)

    x_right, x_left, z_far = at_dp(zh, xr), at_dp(zh, xl), at_dp(1 - zh, x)
    y_right, y_left = at_ex((y + 1) % 4, zl, core), at_ex((y + 3) % 4, zl, core)
    z_near, twin = at_ex(y, 1 - zl, core), at_ex(y, zl, 1 - core)

    counts = dict(send=0, recv=0)

    def semaphore(kind):
        counts[kind] += 1
        return (send_sem if kind == "send" else recv_sem).at[counts[kind] - 1]

    def described(src, dst, send, recv, device):
        return pltpu.make_async_remote_copy(
            src_ref=src, dst_ref=dst, send_sem=send, recv_sem=recv, device_id=device, device_id_type=MESH
        )

    class Landing:
        def __init__(self, ref):
            self.ref, self.semaphore = ref, semaphore("recv")

        def wait(self):
            described(self.ref, self.ref, all_sent[0], self.semaphore, twin).wait_recv()

    class Sent:
        def __init__(self, ref):
            self.ref, self.semaphore = ref, semaphore("send")
            all_sent.append(self.semaphore)

        def wait(self):
            described(self.ref, self.ref, self.semaphore, recv_sem.at[0], twin).wait_send()

    all_sent = []

    def move(src, dst, device, sent, landing):
        return functools.partial(described, src, dst, sent.semaphore, landing.semaphore, device)

    def start(*moves):
        for m in moves:
            for each in m if isinstance(m, tuple) else (m,):
                each().start()

    first, second = pl.ds(0, HALF), pl.ds(HALF, HALF)
    body, routing_rows = (pl.ds(0, TOK),), (pl.ds(TOK, META), pl.ds(0, META_COLS))

    def blocks(n):
        return tokb.at[(pl.ds(0, n), *body)], tokb.at[(pl.ds(0, n), *routing_rows)]

    class Both:
        def __init__(self, kind, n):
            self.tokens, self.routing = (kind(ref) for ref in blocks(n))

        def wait(self):
            self.tokens.wait()
            self.routing.wait()

    tokens_sent = Both(Sent, 15)
    z_in, near_in, across_in, far_in, last_in = (Both(Landing, n) for n in (1, 2, 1, 2, 1))
    twins_in = [Both(Landing, n) for n in (4, 3, 1)]

    def block(src, dst, device, landing, rows=None):
        routing = move(
            tokb.at[(src, *routing_rows)], tokb.at[(dst, *routing_rows)], device, tokens_sent.routing, landing.routing
        )
        if rows is None:
            rows = pl.ds(0, TOK)
        tokens = move(tokb.at[src, rows], tokb.at[dst, rows], device, tokens_sent.tokens, landing.tokens)
        return (tokens,) if rows is second else (routing, tokens)

    t_z = block(OWN, ZED, z_near, z_in)
    t_right, t_left = block(OWN, LEFT, y_right, near_in), block(OWN, RIGHT, y_left, near_in)
    t_fwd_r = block(LEFT, ACROSS, y_right, across_in, first)
    t_fwd_l = block(RIGHT, ACROSS, y_left, across_in, second)
    t_zright, t_zleft = block(ZED, ZLEFT, y_right, far_in), block(ZED, ZRIGHT, y_left, far_in)
    t_zfwd_r = block(ZLEFT, ZACROSS, y_right, last_in, first)
    t_zfwd_l = block(ZRIGHT, ZACROSS, y_left, last_in, second)
    waves = {OWN: 0, ZED: 0, LEFT: 0, RIGHT: 0, ACROSS: 1, ZLEFT: 1, ZRIGHT: 1, ZACROSS: 2}
    twins = {s: block(s, s + 1, twin, twins_in[w]) for s, w in waves.items()}

    class GateUp:
        def __init__(self, p):
            e, n = PIECES[p]
            top, low = pl.ds(0, COL // 2), pl.ds(COL // 2, COL // 2)
            far = 1 - zh

            def shards(k):
                return wg.at[e, n, pl.ds(0, k)]

            self.sent, self.near_in = Sent(shards(7)), Landing(shards(2))
            if p in Z_FIRST:
                self.z_in, self.far_in = Landing(shards(1)), Landing(shards(2))
                self.rest_in = across_in = Landing(shards(2))
                z_in, last_in = self.z_in, self.rest_in
            elif p in X_FIRST:
                self.across_in, self.rest_in = Landing(shards(1)), Landing(shards(4))
                across_in = self.across_in
                z_in = self.far_in = last_in = self.rest_in
            else:
                self.across_in, self.far_in = Landing(shards(1)), Landing(shards(2))
                self.rest_in, across_in = Landing(shards(2)), self.across_in
                z_in = last_in = self.rest_in

            def same(device, z, xx, landing, rows=slice(None)):
                ref = wg.at[e, n, z * 4 + xx, rows]
                return move(ref, ref, device, self.sent, landing)

            self.right, self.left = same(x_right, zh, x, self.near_in), same(x_left, zh, x, self.near_in)
            self.fwd_r, self.fwd_l = same(x_right, zh, xl, across_in, top), same(x_left, zh, xr, across_in, low)
            self.z = same(z_far, zh, x, z_in)
            if p in X_FIRST:
                self.zl, self.zr = same(z_far, zh, xl, self.far_in), same(z_far, zh, xr, self.far_in)
            else:
                self.zright, self.zleft = same(x_right, far, x, self.far_in), same(x_left, far, x, self.far_in)
            if p in X_FIRST:
                self.za = same(z_far, zh, xa, last_in)
            else:
                self.zfwd_r, self.zfwd_l = same(x_right, far, xl, last_in, top), same(x_left, far, xr, last_in, low)

    class Down:
        def __init__(self, half):
            top, low = pl.ds(0, FF // 2), pl.ds(FF // 2, FF // 2)
            cols = pl.ds(half * STEP, STEP)

            def slots(k):
                return wd.at[pl.ds(0, k), :, :, cols]

            self.sent = Sent(slots(7))
            self.near_in, self.across_in, self.z_in, self.far_in, self.last_in = (
                Landing(slots(k)) for k in (2, 1, 1, 2, 1)
            )

            def to(device, src, dst, landing, rows=slice(None)):
                return move(wd.at[src, :, rows, cols], wd.at[dst, :, rows, cols], device, self.sent, landing)

            self.right, self.left = to(x_right, 0, 1, self.near_in), to(x_left, 0, 3, self.near_in)
            self.z = to(z_far, 0, 4, self.z_in)
            self.fwd_r, self.fwd_l = to(x_right, 1, 2, self.across_in, top), to(x_left, 3, 2, self.across_in, low)
            self.zright, self.zleft = to(x_right, 4, 5, self.far_in), to(x_left, 4, 7, self.far_in)
            if half in Z_LAST:
                self.za = to(z_far, 2, 6, self.last_in)
            else:
                self.zfwd_r, self.zfwd_l = to(x_right, 5, 6, self.last_in, top), to(x_left, 7, 6, self.last_in, low)

    gu = [GateUp(p) for p in range(6)]
    dn = [Down(0), Down(1)]

    mine = zh * 4 + x
    def load(src, dst, name):
        pltpu.make_async_copy(src, dst, local_sem.at[name]).start()

    def loaded(dst, name):
        pltpu.make_async_copy(dst, dst, local_sem.at[name]).wait()

    def load_piece(p):
        e, n = PIECES[p]
        load(wgu.at[e, :, pl.ds(n * COL, COL)], wg.at[e, n, mine, :, pl.ds(0, COL)], p)
        load(wgu.at[e, :, pl.ds(FF + n * COL, COL)], wg.at[e, n, mine, :, pl.ds(COL, COL)], p)

    load_piece(4)
    load_piece(5)
    load(tok, tokb.at[OWN, pl.ds(0, TOK)], 6)
    for p in Z_FIRST:
        load_piece(p)
    load(wdn, wd.at[0], 7)

    barrier = pltpu.get_barrier_semaphore()
    for peer in (x_right, x_left, z_far, y_right, y_left, z_near, twin):
        pl.semaphore_signal(barrier, inc=1, device_id=peer, device_id_type=MESH)

    weights = probs[...] / jnp.sum(probs[...], axis=0, keepdims=True)
    high = weights.astype(BF16)
    middle = (weights - high.astype(F32)).astype(BF16)
    low = (weights - high.astype(F32) - middle.astype(F32)).astype(BF16)
    numbers = ids[...].astype(F32).astype(BF16)
    for lane in range(2):
        rows = [v[k : k + 1, :] for v in (numbers, high, middle, low) for k in range(lane, TOP, 2)]
        tokb[OWN, TOK:ROWS, lane * TOK : (lane + 1) * TOK] = jnp.concatenate(rows, axis=0)

    before = lax.broadcasted_iota(jnp.int32, (TOK, TOK), 0)
    after = lax.broadcasted_iota(jnp.int32, (TOK, TOK), 1)
    tri[...] = jnp.where(before < after, 1.0, 0.0).astype(BF16)
    pl.semaphore_wait(barrier, 7)

    slot_number = lax.broadcasted_iota(jnp.int32, (CAP, TOK), 0).astype(F32)

    def dispatch(r, carry):
        routing = tokb[r, pl.ds(TOK, META), pl.ds(0, META_COLS)].astype(F32)
        places, shares = [], []
        for e in range(2):
            number = (ex * 2 + e).astype(F32)
            named = jnp.zeros((1, TOK), F32)
            weight = jnp.zeros((1, TOK), F32)
            for k in range(TOP):
                cols = slice(k % 2 * TOK, (k % 2 + 1) * TOK)
                mark, high, middle, low = (routing[4 * i + k // 2 : 4 * i + k // 2 + 1, cols] for i in range(4))
                hit = mark == number
                value = high + middle + low
                named = named + jnp.where(hit, 1.0, 0.0)
                weight = weight + jnp.where(hit, value, 0.0)
            many = jnp.broadcast_to(named, (16, TOK)).astype(BF16)
            slot = jnp.dot(many, tri[...], preferred_element_type=F32)[0:1, :]
            place = jnp.where(slot_number == slot, jnp.broadcast_to(named, (CAP, TOK)), 0.0)
            places.append(place)
            shares.append(place * weight)
        share = jnp.concatenate(shares, axis=0)
        upper = share.astype(BF16).astype(F32)
        pt[r, :, :] = jnp.concatenate([upper, share - upper], axis=0).T.astype(BF16)
        place = jnp.concatenate(places, axis=0).astype(BF16)
        rows = pl.ds(pl.multiple_of(r * CAP, CAP), CAP)
        for c in range(4):
            cols = slice(c * 512, (c + 1) * 512)
            picked = jnp.dot(place, tokb[r, 0:TOK, cols], preferred_element_type=F32).astype(BF16)
            xs[0, rows, cols] = picked[0:CAP]
            xs[1, rows, cols] = picked[CAP:]
        return carry

    def gate_up(p, *halves):
        e, n = PIECES[p]

        def tile(i, carry):
            rows = pl.ds(pl.multiple_of(i * 640, 640), 640)
            both = jnp.dot(xs[e, rows, :], wg[e, n].reshape(D, 2 * COL), preferred_element_type=F32)
            gate, up = both[:, :COL], both[:, COL:]
            hid[e, rows, n * COL : (n + 1) * COL] = (gate / (1.0 + jnp.exp(-gate)) * up).astype(BF16)
            return carry

        lax.fori_loop(halves[0], halves[-1] + 1, tile, 0)

    def gate_up_part(p, z, rows):
        e, n = PIECES[p]
        width = pl.ds(pl.multiple_of(z * (D // 2), D // 2), D // 2)
        return jnp.dot(
            xs[e, rows, width], wg[e, n, pl.ds(z * 4, 4)].reshape(D // 2, 2 * COL), preferred_element_type=F32
        )

    def gate_up_near(p, half):
        rows = pl.ds(half * 640, 640)
        part[rows, :] = gate_up_part(p, zh, rows)

    def gate_up_far(p):
        e, n = PIECES[p]

        def tile(i, carry):
            rows = pl.ds(pl.multiple_of(i * 640, 640), 640)
            both = part[rows, :] + gate_up_part(p, 1 - zh, rows)
            gate, up = both[:, :COL], both[:, COL:]
            hid[e, rows, n * COL : (n + 1) * COL] = (gate / (1.0 + jnp.exp(-gate)) * up).astype(BF16)
            return carry

        lax.fori_loop(0, 2, tile, 0)

    def own_piece(p):
        e, n = PIECES[p]
        loaded(wg.at[e, n, mine], p)
        start(gu[p].right, gu[p].left)

    def forward(p):
        gu[p].near_in.wait()
        start(gu[p].fwd_r, gu[p].fwd_l)

    def far_start(p):
        gu[p].z_in.wait()
        start(gu[p].zright, gu[p].zleft)

    def far_forward(p):
        gu[p].far_in.wait()
        start(gu[p].zfwd_r, gu[p].zfwd_l)

    own_piece(4)
    loaded(tokb.at[OWN, pl.ds(0, TOK)], 6)
    start(t_z, t_right, t_left, twins[OWN])
    own_piece(5)
    for p in Z_FIRST:
        own_piece(p)
    start(gu[0].z, gu[1].z, gu[4].z)

    forward(4)
    start(gu[4].zl, gu[4].zr, gu[2].z)
    forward(5)
    forward(0)
    near_in.wait()
    start(t_fwd_r, t_fwd_l)
    z_in.wait()
    start(t_zright, t_zleft, twins[ZED], twins[LEFT], twins[RIGHT])
    forward(1)
    forward(2)
    far_start(0)
    forward(3)
    twins_in[0].wait()
    lax.fori_loop(0, 8, dispatch, 0)
    gu[4].across_in.wait()
    start(gu[4].za, gu[3].z, gu[5].z, gu[5].zl, gu[5].zr)
    far_start(1)
    across_in.wait()
    start(twins[ACROSS])
    gu[5].across_in.wait()
    start(gu[5].za)
    gate_up_near(5, 0)
    far_forward(0)
    far_start(2)
    far_in.wait()
    start(t_zfwd_r, t_zfwd_l, twins[ZLEFT], twins[ZRIGHT])
    far_forward(1)
    gu[4].rest_in.wait()
    gate_up(4, 0)
    gu[0].rest_in.wait()
    gate_up(0, 0)
    far_start(3)
    twins_in[1].wait()
    lax.fori_loop(8, 14, dispatch, 0)
    far_forward(2)
    last_in.wait()
    start(twins[ZACROSS])
    gu[1].rest_in.wait()
    gate_up(1, 0)
    twins_in[2].wait()
    lax.fori_loop(14, SRC, dispatch, 0)
    gate_up(4, 1)
    far_forward(3)
    gate_up(0, 1)
    tokens_sent.wait()
    for peer in (y_right, y_left, z_near, twin):
        pl.semaphore_signal(free_sem, inc=1, device_id=peer, device_id_type=MESH)
    loaded(wd.at[0], 7)
    start(dn[0].z, dn[1].z)
    gate_up(1, 1)
    gu[2].rest_in.wait()
    gate_up(2, 0, 1)
    start(dn[0].right, dn[0].left, dn[1].right, dn[1].left)
    gate_up_near(5, 1)
    gu[3].rest_in.wait()
    gate_up(3, 0, 1)
    gu[5].rest_in.wait()
    gate_up_far(5)
    pl.semaphore_wait(free_sem, 4)

    upper, lower = pl.ds(0, TOK // 2), pl.ds(TOK // 2, TOK // 2)
    every = pl.ds(0, TOK)

    class Return:
        def __init__(self, n, slot, half):
            self.n, self.slot, self.half, self.z_first = n, slot, half, n in RETURN_Z_FIRST
            self.width = width = STEP if self.z_first else 2 * STEP
            pair, self.base = n // 2, n % 2 * 8 * STEP
            self.e, self.row = (0, pair * TOK) if pair < 5 else (1, (pair - 3) * TOK)
            self.twin_row = pair % 2 * TOK
            lane = pl.ds(pair % 4 * 512 + n % 2 * 256, width)

            def mine(col, cols, first=0, rows=TOK):
                return xs.at[self.e, pl.ds(self.row + first, rows), pl.ds(self.base + col, cols)]

            if self.z_first:
                self.z_lands = zbuf.at[RETURN_Z_FIRST.index(n)]
                z = (mine(4 * STEP, 4 * STEP), self.z_lands, z_near)
            else:
                z = (mine(STEP, STEP), tokb.at[14, every, pl.ds(n * STEP, STEP)], z_near)
            rows = TOK // 2
            self.twin_lands = tokb.at[pair, every, pl.ds(self.base, 8 * STEP)]
            theirs = xs.at[1, pl.ds(self.twin_row, TOK), pl.ds(self.base, 8 * STEP)]
            self.moves = dict(
                twin=(theirs, self.twin_lands, twin),
                right1=(mine(2 * width, width, 0, rows), tokb.at[8 + n // 8, upper, lane], y_right),
                left1=(mine(2 * width, width, rows, rows), tokb.at[8 + n // 8, lower, lane], y_left),
                right2=(mine(width, width), tokb.at[10 + n // 8, every, lane], y_right),
                left2=(mine(3 * width, width), tokb.at[12 + n // 8, every, lane], y_left),
                z=z,
            )
            self.ring = sums_sent
            self.twin_in, self.hop_in = Landing(self.twin_lands), Landing(tokb.at[8, every, pl.ds(0, width)])
            self.home_in = Landing(tokb.at[10, every, pl.ds(0, 2 * width)])
            self.z_in = Landing(z[1])
            self.landings = dict(
                twin=self.twin_in, right1=self.hop_in, left1=self.hop_in, right2=self.home_in, left2=self.home_in, z=self.z_in
            )
            column = (((zh + slot // 4) % 2) * 4 + (x + 4 - slot % 4) % 4) * COL + half * STEP
            self.store = pltpu.make_async_copy(
                ob.at[n], out.at[:, pl.ds(pl.multiple_of(column, STEP), STEP)], out_sem
            )

        def start(self, *names):
            for name in names:
                src, dst, device = self.moves[name]
                sent = twins_sent[self.n % 4] if name == "twin" else sums_sent
                start(move(src, dst, device, sent, self.landings[name]))

        def landed(self, name):
            return self.moves[name][1][...].astype(F32)

        def sums(self, col, cols, first=0, rows=TOK):
            return xs[self.e, self.row + first : self.row + first + rows, self.base + col : self.base + col + cols].astype(F32)

        def keep(self, total, col, first=0):
            rows, cols = total.shape
            at = slice(self.row + first, self.row + first + rows)
            xs[self.e, at, self.base + col : self.base + col + cols] = total.astype(BF16)

        def add(self, theirs, cols):
            def some(i, carry):
                at = pl.ds(pl.multiple_of(self.row + i * 64, 64), 64)
                got = theirs[pl.ds(pl.multiple_of(i * 64, 64), 64), :].astype(F32)
                lanes = slice(self.base, self.base + cols)
                xs[self.e, at, lanes] = (xs[self.e, at, lanes].astype(F32) + got).astype(BF16)
                return carry

            lax.fori_loop(0, TOK // 64, some, 0)

        def join_twin(self):
            self.twin_in.wait()
            self.add(self.twin_lands, 8 * STEP)
            self.start(*(("z",) if self.z_first else ("right1", "left1")))

        def second(self):
            width, rows = self.width, TOK // 2
            self.hop_in.wait()
            for there, col, first in (("right", width, 0), ("left", 3 * width, rows)):
                self.keep(self.sums(col, width, first, rows) + self.landed(there + "1"), col, first)
                self.start(there + "2")

        def home(self):
            self.home_in.wait()
            return self.sums(0, self.width) + self.landed("right2") + self.landed("left2")

        def hop(self):
            if self.z_first:
                self.z_in.wait()
                self.add(self.z_lands, 4 * STEP)
                self.start("right1", "left1")
            else:
                self.second()

        def third(self):
            if self.z_first:
                self.second()
            else:
                self.keep(self.home(), 0)
                self.start("z")

        def last(self):
            if self.z_first:
                total = self.home()
            else:
                self.z_in.wait()
                total = self.sums(0, STEP) + self.landed("z")
            ob[self.n] = total.astype(BF16)
            self.store.start()

    sums_sent = Sent(xs.at[:, pl.ds(0, STEPS * TOK // 4), pl.ds(0, 14 * STEP)])
    twins_sent = [Sent(xs.at[1, pl.ds(0, TOK), pl.ds(0, 8 * STEP)]) for _ in range(4)]
    returns, unit_steps = [], []
    for unit in UNITS:
        unit_steps.append([Return(len(returns) + i, slot, half) for i, (slot, half) in enumerate(unit)])
        returns += unit_steps[-1]

    def combine(steps):
        cols = len(steps) * STEP

        def side(mine, carry):
            def where(step):
                row = (1 - mine) * step.twin_row + mine * step.row
                return (1 - mine) + mine * step.e, pl.ds(pl.multiple_of(row, TOK), TOK)

            for (yy, zz), s in RETURN.items():
                r = s + 1 - mine
                total = jnp.dot(pt[r], yb[r, :, 0:cols], preferred_element_type=F32).astype(BF16)
                for i, step in enumerate(steps):
                    place = 4 * zz + yy if step.z_first else 2 * yy + zz
                    e, rows = where(step)
                    at = slice(step.base + place * STEP, step.base + (place + 1) * STEP)
                    xs[e, rows, at] = total[:, i * STEP : (i + 1) * STEP]

            @pl.when(mine == 0)
            def _():
                for step in steps:
                    step.start("twin")

            return carry

        lax.fori_loop(0, 2, side, 0)

    def compute(u):
        steps, unit = unit_steps[u], UNITS[u]
        for step in steps:
            if step.n >= 4:
                twins_sent[step.n % 4].wait()
        for slot, half in unit:
            if slot in (1, 3):
                once("n", half)
            elif slot == 2:
                once("a", half)
            elif slot == 4:
                once("f", half)
            elif slot in (5, 7):
                once("w", half)
            elif slot == 6:
                once("A", half)
        for e in range(2):
            shard = jnp.concatenate([wd[slot, e, :, half * STEP : (half + 1) * STEP] for slot, half in unit], axis=1)
            y_e = jnp.dot(hid[e], shard, preferred_element_type=F32).astype(BF16)
            for part_at in (0, 2 * CAP):
                rows = slice(part_at + e * CAP, part_at + (e + 1) * CAP)
                yb[:, rows, 0 : len(unit) * STEP] = y_e.reshape(SRC, CAP, -1)
        combine(steps)

    made = set()

    def once(what, half):
        if (what, half) in made:
            return
        made.add((what, half))
        d = dn[half]
        if what == "n":
            d.near_in.wait()
            start(d.fwd_r, d.fwd_l)
        elif what == "a":
            once("n", half)
            d.across_in.wait()
        elif what == "f":
            d.z_in.wait()
            start(d.zright, d.zleft)
        elif what == "w":
            once("f", half)
            d.far_in.wait()
        elif what == "F":
            once("w", half)
            start(d.zfwd_r, d.zfwd_l)
        elif what == "g":
            once("a", half)
            start(d.za)
        elif what == "A":
            once("g" if half in Z_LAST else "F", half)
            d.last_in.wait()

    do = {
        "C": compute, "T": lambda n: returns[n].join_twin(), "S": lambda n: returns[n].hop(),
        "H": lambda n: returns[n].third(), "L": lambda n: returns[n].last(),
        **{what: functools.partial(once, what) for what in "nfFg"},
    }
    for what, n in PLAN:
        do[what](n)
    sums_sent.wait()
    for n in range(STEPS - 4, STEPS):
        twins_sent[n % 4].wait()
    pltpu.make_async_copy(ob, ob, out_sem).wait()
    for group in (*gu, *dn):
        group.sent.wait()


def shards(tokens, expert_ids, route_probs, w_gate_up, w_down):
    any_spec = pl.BlockSpec(memory_space=pl.ANY)
    vmem_spec = pl.BlockSpec(memory_space=pltpu.VMEM)
    return pl.pallas_call(
        kernel,
        out_shape=jax.ShapeDtypeStruct((TOK, D), BF16),
        in_specs=[any_spec, vmem_spec, vmem_spec, any_spec, any_spec],
        out_specs=any_spec,
        scratch_shapes=[
            pltpu.VMEM((SRC, ROWS, D), BF16),
            pltpu.VMEM((2, 3, SHARDS, COL, 2 * COL), BF16),
            pltpu.VMEM((SHARDS, 2, FF, COL), BF16),
            pltpu.VMEM((2, SRC * CAP, D), BF16),
            pltpu.VMEM((2, SRC * CAP, FF), BF16),
            pltpu.VMEM((SRC, TOK, 4 * CAP), BF16),
            pltpu.VMEM((SRC, 4 * CAP, COL), BF16),
            pltpu.VMEM((TOK, TOK), BF16),
            pltpu.VMEM((len(RETURN_Z_FIRST), TOK, 4 * STEP), BF16),
            pltpu.VMEM((STEPS, TOK, STEP), BF16),
            pltpu.VMEM((SRC * CAP, 2 * COL), F32),
            pltpu.SemaphoreType.DMA((8,)),
            pltpu.SemaphoreType.DMA((SENDS,)),
            pltpu.SemaphoreType.DMA((LANDINGS,)),
            pltpu.SemaphoreType.DMA,
            pltpu.SemaphoreType.REGULAR,
        ],
        compiler_params=pltpu.CompilerParams(
            collective_id=0, has_side_effects=True, vmem_limit_bytes=67_000_000
        ),
    )(tokens, expert_ids.T, route_probs.T, w_gate_up, w_down)


def solution(mesh):
    spec = P(("dp", "expert"), None)
    in_specs = (spec, spec, spec, P("expert", "dp", None), P("expert", None, "dp"))
    return jax.shard_map(shards, mesh=mesh, in_specs=in_specs, out_specs=spec, check_vma=False)
```
